512 devices in a mesh: ty: 32 (over y, x_hi, core), tx: 16 (over z, x_lo).
Axes of the slice: x: 4 (x_hi: 2, x_lo: 2; x = x_hi * 2 + x_lo), y: 8, z: 8, core: 2. Of those that a mesh axis runs over, the one named last changes fastest.
Arguments:
- noise: float32 [4096, 4096], P('ty', 'tx'), may hold values from -6 to 6
- root_spectrum: float32 [384, 512], replicated, may hold values from 0.25 to 4
Outputs:
- field: float32 [4096, 4096], P('ty', 'tx')
The draws below stay inside these ranges and needn't reach their ends.
All inputs are finite; a program needn't handle non-finite values.
Results may differ from the reference program's by a relative error of at most 0.0003.
Values sent between devices are 32-bit elements; how exact they have to be, the bound alone decides.
A program may use at most 64 MiB of HBM per device.

```python
import math
import jax
import jax.numpy as jnp
from jax import lax

MARGIN = 128
CY = 128
CX = 256
EY = 384
EX = 512
NY = 4096
NX = 4096
N_TY = 32
N_TX = 16


def block_levels(own_key, dims, cuts, smallest, top_value):
    def one(dim, shards_of):
        draws = jax.random.uniform(jax.random.fold_in(jax.random.fold_in(own_key, 6), dim), (shards_of,), jnp.float32, smallest / len(cuts), top_value / len(cuts))
        return jnp.repeat(jnp.exp(draws), dims[dim] // shards_of).reshape((-1,) + (1,) * (len(dims) - dim - 1))

    factor_of = one(*cuts[0])
    for cut in cuts[1:]:
        factor_of = factor_of * one(*cut)
    return factor_of


def normal_values(stream_key, shape, deviation, reach, split=(), kind=jnp.bfloat16):
    level = block_levels(stream_key, shape, split, -0.22, 0.18) if split else 1.0
    values = jax.random.normal(stream_key, shape, jnp.float32) * deviation * level
    return jnp.minimum(jnp.maximum(values, -reach), reach).astype(kind)


def setup_inputs(seed: int = 0) -> dict:
    key_list = jax.random.split(jax.random.key(seed), 3)
    return {
        "noise": normal_values(key_list[0], (NY, NX), 1.0, 6.0, ((0, 32), (1, 16)), jnp.float32),
        "root_spectrum": jnp.clip(jnp.exp(jax.random.uniform(key_list[1], (EY, EX), jnp.float32, math.log(0.25), math.log(4.0))), 0.25, 4.0),
    }


def blend_weights(margin, rows_total, cols_total):
    knots = (jnp.arange(rows_total, dtype=jnp.float32) + 0.5) / margin
    weight_rows = jnp.where(knots < 1.0, 0.5 * knots * knots,
                            jnp.where(knots < 2.0, 0.5 * (-2.0 * knots * knots + 6.0 * knots - 3.0),
                                      0.5 * (3.0 - knots) * (3.0 - knots)))
    columns = jnp.arange(cols_total, dtype=jnp.float32) + 0.5
    weight_cols = 1.0 - jnp.abs(columns - 2.0 * margin) / (2.0 * margin)
    return weight_rows[:, None] * weight_cols[None, :]


def reference(noise, root_spectrum):
    margin = MARGIN
    padded = jnp.pad(noise, ((margin, margin), (margin, margin)), mode="wrap")
    weights = blend_weights(margin, EY, EX)

    def place(total, counter):
        row_tile = (counter // N_TX).astype(jnp.int32)
        col_tile = (counter % N_TX).astype(jnp.int32)
        start_row = (row_tile * CY).astype(jnp.int32)
        start_col = (col_tile * CX).astype(jnp.int32)
        window = lax.dynamic_slice(padded, (start_row, start_col), (EY, EX))
        sample = jnp.real(jnp.fft.ifft2(root_spectrum * jnp.fft.fft2(window)))
        blended = sample * weights
        current = lax.dynamic_slice(total, (start_row, start_col), (EY, EX))
        total = lax.dynamic_update_slice(total, current + blended, (start_row, start_col))
        return total, None

    start = jnp.zeros(padded.shape, padded.dtype)
    total, _ = lax.scan(place, start, jnp.arange(N_TY * N_TX, dtype=jnp.int32))
    folded = total[margin:margin + NY]
    folded = folded.at[NY - margin:].add(total[:margin])
    folded = folded.at[:margin].add(total[margin + NY:])
    result = folded[:, margin:margin + NX]
    result = result.at[:, NX - margin:].add(folded[:, :margin])
    result = result.at[:, :margin].add(folded[:, margin + NX:])
    return result
```

```python
import functools
import math

import jax
import jax.numpy as jnp
import numpy as np
from jax import lax
from jax.experimental import pallas as pl
from jax.experimental.pallas import tpu as pltpu
from jax.sharding import PartitionSpec as P

MARGIN = 128
EY = 384
EX = 512
BLOCK = 256
HALF_Y = EY // 2
HALF_X = EX // 2
MESH = pl.DeviceIdType.MESH


def split_table(table):
    high = table.astype(jnp.bfloat16)
    low = (table - high.astype(np.float64)).astype(jnp.bfloat16)
    return np.stack([high, low])


def row_basis():
    ky = np.arange(HALF_Y)[:, None]
    y = np.arange(EY)[None, :]
    angle = 2.0 * math.pi * (ky * y % EY) / EY
    lower = -np.sin(angle)
    lower[0] = np.cos(math.pi * np.arange(EY))
    return np.concatenate([np.cos(angle), lower])


def column_basis():
    x = np.arange(HALF_X)[:, None]
    bases = []
    for odd in (0, 1):
        kx = 2 * np.arange(HALF_X // 2)[None, :] + odd
        angle = 2.0 * math.pi * (kx * x % EX) / EX
        sine = np.sin(angle)
        if not odd:
            sine[:, 0] = np.cos(math.pi * np.arange(HALF_X))
        bases.append(np.concatenate([np.cos(angle), sine], axis=1))
    return np.stack(bases)


def row_weights():
    knots = (np.arange(EY) + 0.5) / MARGIN
    return np.where(
        knots < 1.0,
        0.5 * knots * knots,
        np.where(
            knots < 2.0,
            0.5 * (-2.0 * knots * knots + 6.0 * knots - 3.0),
            0.5 * (3.0 - knots) * (3.0 - knots),
        ),
    )


def tables():
    rows = row_basis()
    forward = split_table(rows)
    forward = forward.reshape(2, EY, 3, MARGIN).transpose(2, 0, 1, 3)
    back = split_table((rows * row_weights()[None, :]).T)
    back = back.reshape(2, 3, MARGIN, EY).transpose(1, 0, 2, 3)
    columns = split_table(column_basis())
    return np.ascontiguousarray(forward), np.ascontiguousarray(back), columns


def split(value):
    high = value.astype(jnp.bfloat16)
    return high, (value - high.astype(jnp.float32)).astype(jnp.bfloat16)


def dot(left, right):
    return jnp.dot(left, right, preferred_element_type=jnp.float32)


def dot_t(left, right):
    return lax.dot_general(left, right, (((1,), (1,)), ((), ())), preferred_element_type=jnp.float32)


def three(product, left, right):
    return product(left[0], right[0]) + product(left[0], right[1]) + product(left[1], right[0])


def iota(shape, dim):
    return lax.broadcasted_iota(jnp.int32, shape, dim)


def indicator(condition):
    return jnp.where(condition, 1.0, 0.0)


def spectrum_terms(spectrum, even_ref, cross_ref):
    source = iota((EX, 128), 0)
    lane = iota((EX, 128), 1)
    folds = []
    for sign in (1.0, -1.0):
        for odd in (0, 1):
            kx = 2 * lane + odd
            fold = indicator(source == kx) + sign * indicator(source == EX - kx)
            if sign < 0 and not odd:
                fold = jnp.where(lane == 0, indicator(source == HALF_X), fold)
            folds.append(fold)
    fold = jnp.concatenate(folds, axis=1).astype(jnp.bfloat16)
    high, low = split(spectrum * (1.0 / (EY * EX)))
    folded = dot(high, fold) + dot(low, fold)
    high, low = split(folded)
    ky = iota((HALF_Y, EY), 0)
    row = iota((HALF_Y, EY), 1)
    straight = indicator(row == ky)
    mirrored = indicator(row == EY - ky)
    sums = (straight + mirrored).astype(jnp.bfloat16)
    gaps = jnp.where(ky == 0, 0.0, straight - mirrored).astype(jnp.bfloat16)
    even = dot(sums, high[:, :384]) + dot(sums, low[:, :384])
    cross = dot(gaps, high[:, 256:]) + dot(gaps, low[:, 256:])
    first_row = iota((HALF_Y, 128), 0) == 0
    first_lane = iota((HALF_Y, 128), 1) == 0
    middle = folded[HALF_Y : HALF_Y + 1]
    for slot, group in ((0, 0), (1, 0), (2, 1), (3, 1)):
        upper = even[:, 128 * group : 128 * group + 128]
        edge = jnp.broadcast_to(middle[:, 128 * group : 128 * group + 128], (HALF_Y, 128))
        if slot == 1:
            upper = jnp.where(first_lane, even[:, 256:384], upper)
            edge = jnp.where(first_lane, jnp.broadcast_to(middle[:, 256:384], (HALF_Y, 128)), edge)
        even_ref[0:HALF_Y, pl.ds(128 * slot, 128)] = upper
        even_ref[HALF_Y:EY, pl.ds(128 * slot, 128)] = jnp.where(first_row, edge, upper)
    cross_ref[:, 0:128] = jnp.where(first_lane, 0.0, cross[:, :128])
    cross_ref[:, 128:256] = cross[:, 128:]


def kernel(
    n_ty,
    n_tx,
    noise_ref,
    spectrum_ref,
    forward_ref,
    back_ref,
    columns_ref,
    out_ref,
    window,
    spectrum,
    forward,
    back,
    columns,
    even,
    cross,
    staged,
    blended,
    side,
    from_remote,
    from_sibling,
    from_side,
    from_corner,
    local_sem,
    send_sem,
    recv_sem,
):
    me_y = lax.axis_index("ty")
    me_x = lax.axis_index("tx")
    core = lax.rem(me_y, 2)
    sibling_y = me_y + 1 - 2 * core
    remote_y = lax.rem(me_y + 2 * core - 1 + n_ty, n_ty)
    left_x = lax.rem(me_x + n_tx - 1, n_tx)
    right_x = lax.rem(me_x + 1, n_tx)

    sibling = (sibling_y, me_x)
    remote = (remote_y, me_x)
    left = (me_y, left_x)
    right = (me_y, right_x)
    corner_left = (remote_y, left_x)
    corner_right = (remote_y, right_x)
    partners = (remote, corner_left, corner_right, left, right, sibling)

    barrier = pltpu.get_barrier_semaphore()
    for partner in partners:
        pl.semaphore_signal(barrier, inc=1, device_id=partner, device_id_type=MESH)

    def local(source, target, index):
        copy = pltpu.make_async_copy(source, target, local_sem.at[index])
        copy.start()
        return copy

    own = window.at[1, :, pl.ds(MARGIN, BLOCK)]
    load_noise = local(noise_ref, own, 0)
    load_spectrum = local(spectrum_ref, spectrum, 1)
    slots = (2 * core, 1, 2 - 2 * core)
    load_tables = [local(forward_ref.at[slots[i]], forward.at[i], 2 + i) for i in range(3)]
    load_columns = local(columns_ref, columns, 5)
    load_back = [local(back_ref.at[slots[i]], back.at[i], 6 + i) for i in range(3)]

    load_noise.wait()
    pl.semaphore_wait(barrier, len(partners))

    def send(source, target, index, device):
        copy = pltpu.make_async_remote_copy(
            src_ref=source,
            dst_ref=target,
            send_sem=send_sem.at[index],
            recv_sem=recv_sem.at[index],
            device_id=device,
            device_id_type=MESH,
        )
        copy.start()
        return copy

    left_strip = pl.ds(0, MARGIN)
    left_half = pl.ds(MARGIN, MARGIN)
    right_half = pl.ds(2 * MARGIN, MARGIN)
    right_strip = pl.ds(3 * MARGIN, MARGIN)
    centre = pl.ds(MARGIN, BLOCK)

    to_right = send(window.at[1, :, right_half], window.at[1, :, left_strip], 0, right)
    to_left = send(window.at[1, :, left_half], window.at[1, :, right_strip], 1, left)
    to_remote = send(own, window.at[0, :, centre], 2, remote)
    to_corner_right = send(window.at[1, :, right_half], window.at[0, :, left_strip], 3, corner_right)
    to_corner_left = send(window.at[1, :, left_half], window.at[0, :, right_strip], 4, corner_left)
    to_sibling = send(own, window.at[2, :, centre], 5, sibling)

    load_spectrum.wait()
    spectrum_terms(spectrum[...], even, cross)
    for load in load_tables:
        load.wait()
    load_columns.wait()

    to_right.wait_recv()
    pass_left = send(window.at[1, :, left_strip], window.at[2, :, left_strip], 6, sibling)
    to_left.wait_recv()
    pass_right = send(window.at[1, :, right_strip], window.at[2, :, right_strip], 7, sibling)
    to_sibling.wait_recv()
    pass_left.wait_recv()
    pass_right.wait_recv()

    near = split(window[1:3].reshape(2 * MARGIN, EX))
    near_tables = [jnp.concatenate([forward[1, i], forward[2, i]], axis=1) for i in range(2)]
    staged[...] = three(dot, near_tables, near)
    to_remote.wait_recv()
    to_corner_right.wait_recv()
    to_corner_left.wait_recv()
    far = split(window[0])
    rows = staged[...] + three(dot, (forward[0, 0], forward[0, 1]), far)

    halves = []
    for parity in range(2):
        lower, upper = rows[:, :HALF_X], rows[:, HALF_X:]
        folded = lower + upper if parity == 0 else lower - upper
        waves = three(dot, split(folded), (columns[0, parity], columns[1, parity]))
        mixed = cross[:, pl.ds(128 * parity, 128)]
        scale = even[:, pl.ds(256 * parity, 256)]
        flat = waves * scale
        real_c, real_s = waves[:HALF_Y, :128], waves[:HALF_Y, 128:]
        imag_c, imag_s = waves[HALF_Y:, :128], waves[HALF_Y:, 128:]
        shift = jnp.concatenate(
            [
                jnp.concatenate([mixed * imag_s, -(mixed * imag_c)], axis=1),
                jnp.concatenate([-(mixed * real_s), mixed * real_c], axis=1),
            ],
            axis=0,
        )
        halves.append(three(dot_t, split(flat + shift), (columns[0, parity], columns[1, parity])))
    position = iota((1, HALF_X), 1).astype(jnp.float32) + 0.5
    rising = position * (1.0 / HALF_X)
    falling = 1.0 - rising
    strips = jnp.concatenate(
        [(halves[0] + halves[1]) * rising, (halves[0] - halves[1]) * falling], axis=1
    )
    strips = split(strips)

    for load in load_back:
        load.wait()
    blended[0] = three(dot, (back[0, 0], back[0, 1]), strips)
    add_remote = send(blended.at[0, :, centre], from_remote, 8, remote)
    add_corner_left = send(blended.at[0, :, left_strip], from_corner.at[1], 9, corner_left)
    add_corner_right = send(blended.at[0, :, right_strip], from_corner.at[0], 10, corner_right)
    blended[2] = three(dot, (back[2, 0], back[2, 1]), strips)
    add_sibling = send(blended.at[2], from_sibling, 11, sibling)
    blended[1] = three(dot, (back[1, 0], back[1, 1]), strips)
    add_sibling.wait_recv()
    side[0] = blended[1, :, left_strip] + from_sibling[:, left_strip]
    add_left = send(side.at[0], from_side.at[1], 12, left)
    side[1] = blended[1, :, right_strip] + from_sibling[:, right_strip]
    add_right = send(side.at[1], from_side.at[0], 13, right)
    middle = blended[1, :, centre] + from_sibling[:, centre]
    add_remote.wait_recv()
    middle = middle + from_remote[...]
    add_corner_left.wait_recv()
    add_corner_right.wait_recv()
    corners = jnp.concatenate([from_corner[0], from_corner[1]], axis=1)
    middle = middle + corners
    add_left.wait_recv()
    add_right.wait_recv()
    out_ref[...] = middle + jnp.concatenate([from_side[0], from_side[1]], axis=1)
    for copy in (
        to_right,
        to_left,
        to_remote,
        to_corner_right,
        to_corner_left,
        to_sibling,
        pass_left,
        pass_right,
        add_remote,
        add_corner_left,
        add_corner_right,
        add_sibling,
        add_left,
        add_right,
    ):
        copy.wait_send()


def per_device(n_ty, n_tx, noise, root_spectrum):
    forward, back, columns = tables()
    anywhere = pl.BlockSpec(memory_space=pl.ANY)
    f32 = jnp.float32
    bf16 = jnp.bfloat16
    return pl.pallas_call(
        functools.partial(kernel, n_ty, n_tx),
        out_shape=jax.ShapeDtypeStruct(noise.shape, f32),
        in_specs=[anywhere] * 5,
        out_specs=pl.BlockSpec(memory_space=pltpu.VMEM),
        scratch_shapes=[
            pltpu.VMEM((3, MARGIN, EX), f32),
            pltpu.VMEM((EY, EX), f32),
            pltpu.VMEM((3, 2, EY, MARGIN), bf16),
            pltpu.VMEM((3, 2, MARGIN, EY), bf16),
            pltpu.VMEM((2, 2, HALF_X, HALF_X), bf16),
            pltpu.VMEM((EY, EX), f32),
            pltpu.VMEM((HALF_Y, HALF_X), f32),
            pltpu.VMEM((EY, EX), f32),
            pltpu.VMEM((3, MARGIN, EX), f32),
            pltpu.VMEM((2, MARGIN, MARGIN), f32),
            pltpu.VMEM((MARGIN, BLOCK), f32),
            pltpu.VMEM((MARGIN, EX), f32),
            pltpu.VMEM((2, MARGIN, MARGIN), f32),
            pltpu.VMEM((2, MARGIN, MARGIN), f32),
            pltpu.SemaphoreType.DMA((9,)),
            pltpu.SemaphoreType.DMA((14,)),
            pltpu.SemaphoreType.DMA((14,)),
        ],
        compiler_params=pltpu.CompilerParams(collective_id=0, has_side_effects=True),
        name="field_tile",
    )(noise, root_spectrum, jnp.asarray(forward), jnp.asarray(back), jnp.asarray(columns))


def solution(mesh):
    placed = (P("ty", "tx"), P())
    body = functools.partial(per_device, mesh.shape["ty"], mesh.shape["tx"])
    return jax.shard_map(
        body, mesh=mesh, in_specs=placed, out_specs=P("ty", "tx"), check_vma=False
    )
```

```python
import functools
import math

import jax
import jax.numpy as jnp
import numpy as np
from jax import lax
from jax.experimental import pallas as pl
from jax.experimental.pallas import tpu as pltpu
from jax.sharding import PartitionSpec as P

MARGIN = 128
EY = 384
EX = 512
BLOCK = 256
HALF_Y = EY // 2
HALF_X = EX // 2
MESH = pl.DeviceIdType.MESH


def split_table(table):
    high = table.astype(jnp.bfloat16)
    low = (table - high.astype(np.float64)).astype(jnp.bfloat16)
    return np.stack([high, low])


def row_basis():
    ky = np.arange(HALF_Y)[:, None]
    y = np.arange(EY)[None, :]
    angle = 2.0 * math.pi * (ky * y % EY) / EY
    lower = -np.sin(angle)
    lower[0] = np.cos(math.pi * np.arange(EY))
    return np.concatenate([np.cos(angle), lower])


def column_basis():
    x = np.arange(HALF_X)[:, None]
    bases = []
    for odd in (0, 1):
        kx = 2 * np.arange(HALF_X // 2)[None, :] + odd
        angle = 2.0 * math.pi * (kx * x % EX) / EX
        sine = np.sin(angle)
        if not odd:
            sine[:, 0] = np.cos(math.pi * np.arange(HALF_X))
        bases.append(np.concatenate([np.cos(angle), sine], axis=1))
    return np.stack(bases)


def row_weights():
    knots = (np.arange(EY) + 0.5) / MARGIN
    return np.where(
        knots < 1.0,
        0.5 * knots * knots,
        np.where(
            knots < 2.0,
            0.5 * (-2.0 * knots * knots + 6.0 * knots - 3.0),
            0.5 * (3.0 - knots) * (3.0 - knots),
        ),
    )


def tables():
    rows = row_basis()
    forward = split_table(rows)
    forward = forward.reshape(2, EY, 3, MARGIN).transpose(2, 0, 1, 3)
    back = split_table((rows * row_weights()[None, :]).T)
    back = back.reshape(2, 3, MARGIN, EY).transpose(1, 0, 2, 3)
    columns = split_table(column_basis())
    return np.ascontiguousarray(forward), np.ascontiguousarray(back), columns


def split(value):
    high = value.astype(jnp.bfloat16)
    return high, (value - high.astype(jnp.float32)).astype(jnp.bfloat16)


def dot(left, right):
    return jnp.dot(left, right, preferred_element_type=jnp.float32)


def dot_t(left, right):
    return lax.dot_general(left, right, (((1,), (1,)), ((), ())), preferred_element_type=jnp.float32)


def three(product, left, right):
    return product(left[0], right[0]) + product(left[0], right[1]) + product(left[1], right[0])


def iota(shape, dim):
    return lax.broadcasted_iota(jnp.int32, shape, dim)


def indicator(condition):
    return jnp.where(condition, 1.0, 0.0)


def fold_columns(spectrum):
    source = iota((EX, 128), 0)
    lane = iota((EX, 128), 1)
    folds = []
    for sign in (1.0, -1.0):
        for odd in (0, 1):
            kx = 2 * lane + odd
            fold = indicator(source == kx) + sign * indicator(source == EX - kx)
            if sign < 0 and not odd:
                fold = jnp.where(lane == 0, indicator(source == HALF_X), fold)
            folds.append(fold)
    fold = jnp.concatenate(folds, axis=1).astype(jnp.bfloat16)
    high, low = split(spectrum * (1.0 / (EY * EX)))
    return dot(high, fold) + dot(low, fold)


def fold_rows(folded, even_ref, cross_ref):
    high, low = split(folded)
    ky = iota((HALF_Y, EY), 0)
    row = iota((HALF_Y, EY), 1)
    straight = indicator(row == ky)
    mirrored = indicator(row == EY - ky)
    sums = (straight + mirrored).astype(jnp.bfloat16)
    gaps = jnp.where(ky == 0, 0.0, straight - mirrored).astype(jnp.bfloat16)
    even = dot(sums, high[:, :384]) + dot(sums, low[:, :384])
    cross = dot(gaps, high[:, 256:]) + dot(gaps, low[:, 256:])
    first_row = iota((HALF_Y, 128), 0) == 0
    first_lane = iota((HALF_Y, 128), 1) == 0
    middle = folded[HALF_Y : HALF_Y + 1]
    for slot, group in ((0, 0), (1, 0), (2, 1), (3, 1)):
        upper = even[:, 128 * group : 128 * group + 128]
        edge = jnp.broadcast_to(middle[:, 128 * group : 128 * group + 128], (HALF_Y, 128))
        if slot == 1:
            upper = jnp.where(first_lane, even[:, 256:384], upper)
            edge = jnp.where(first_lane, jnp.broadcast_to(middle[:, 256:384], (HALF_Y, 128)), edge)
        even_ref[0:HALF_Y, pl.ds(128 * slot, 128)] = upper
        even_ref[HALF_Y:EY, pl.ds(128 * slot, 128)] = jnp.where(first_row, edge, upper)
    cross_ref[:, 0:128] = jnp.where(first_lane, 0.0, cross[:, :128])
    cross_ref[:, 128:256] = cross[:, 128:]


def kernel(
    n_ty,
    n_tx,
    noise_ref,
    spectrum_ref,
    forward_ref,
    back_ref,
    columns_ref,
    out_ref,
    window,
    spectrum,
    forward,
    back,
    columns,
    even,
    cross,
    staged,
    blended,
    side,
    from_remote,
    from_sibling,
    from_side,
    from_corner,
    local_sem,
    send_sem,
    recv_sem,
):
    me_y = lax.axis_index("ty")
    me_x = lax.axis_index("tx")
    core = lax.rem(me_y, 2)
    sibling_y = me_y + 1 - 2 * core
    remote_y = lax.rem(me_y + 2 * core - 1 + n_ty, n_ty)
    left_x = lax.rem(me_x + n_tx - 1, n_tx)
    right_x = lax.rem(me_x + 1, n_tx)

    sibling = (sibling_y, me_x)
    remote = (remote_y, me_x)
    left = (me_y, left_x)
    right = (me_y, right_x)
    corner_left = (remote_y, left_x)
    corner_right = (remote_y, right_x)
    partners = (remote, corner_left, corner_right, left, right, sibling)

    barrier = pltpu.get_barrier_semaphore()
    for partner in partners:
        pl.semaphore_signal(barrier, inc=1, device_id=partner, device_id_type=MESH)

    def local(source, target, index):
        copy = pltpu.make_async_copy(source, target, local_sem.at[index])
        copy.start()
        return copy

    own = window.at[1, :, pl.ds(MARGIN, BLOCK)]
    load_noise = local(noise_ref, own, 0)
    load_spectrum = local(spectrum_ref, spectrum, 1)
    slots = (2 * core, 1, 2 - 2 * core)
    load_tables = [local(forward_ref.at[slots[i]], forward.at[i], 2 + i) for i in range(3)]
    load_columns = local(columns_ref, columns, 5)
    load_back = [local(back_ref.at[slots[i]], back.at[i], 6 + i) for i in range(3)]

    load_noise.wait()
    load_spectrum.wait()
    folded = fold_columns(spectrum[...])
    spectrum[...] = folded
    pl.semaphore_wait(barrier, len(partners))

    def send(source, target, index, device):
        copy = pltpu.make_async_remote_copy(
            src_ref=source,
            dst_ref=target,
            send_sem=send_sem.at[index],
            recv_sem=recv_sem.at[index],
            device_id=device,
            device_id_type=MESH,
        )
        copy.start()
        return copy

    left_strip = pl.ds(0, MARGIN)
    left_half = pl.ds(MARGIN, MARGIN)
    right_half = pl.ds(2 * MARGIN, MARGIN)
    right_strip = pl.ds(3 * MARGIN, MARGIN)
    centre = pl.ds(MARGIN, BLOCK)

    to_right = send(window.at[1, :, right_half], window.at[1, :, left_strip], 0, right)
    to_left = send(window.at[1, :, left_half], window.at[1, :, right_strip], 1, left)
    to_remote = send(own, window.at[0, :, centre], 2, remote)
    to_corner_right = send(window.at[1, :, right_half], window.at[0, :, left_strip], 3, corner_right)
    to_corner_left = send(window.at[1, :, left_half], window.at[0, :, right_strip], 4, corner_left)
    to_sibling = send(own, window.at[2, :, centre], 5, sibling)

    fold_rows(spectrum[...], even, cross)
    for load in load_tables:
        load.wait()
    load_columns.wait()

    def to_waves(rows):
        lower, upper = rows[:, :HALF_X], rows[:, HALF_X:]
        return jnp.concatenate(
            [
                three(dot, split(lower + upper), (columns[0, 0], columns[1, 0])),
                three(dot, split(lower - upper), (columns[0, 1], columns[1, 1])),
            ],
            axis=1,
        )

    position = iota((1, HALF_X), 1).astype(jnp.float32) + 0.5
    rising = position * (1.0 / HALF_X)
    falling = 1.0 - rising

    def from_waves(waves):
        straight = three(dot_t, split(waves[:, :HALF_X]), (columns[0, 0], columns[1, 0]))
        turned = three(dot_t, split(waves[:, HALF_X:]), (columns[0, 1], columns[1, 1]))
        return (straight + turned) * rising, (straight - turned) * falling

    to_right.wait_recv()
    pass_left = send(window.at[1, :, left_strip], window.at[2, :, left_strip], 6, sibling)
    to_left.wait_recv()
    pass_right = send(window.at[1, :, right_strip], window.at[2, :, right_strip], 7, sibling)
    own_waves = split(to_waves(window[1]))
    staged[...] = three(dot, (forward[1, 0], forward[1, 1]), own_waves)
    to_sibling.wait_recv()
    pass_left.wait_recv()
    pass_right.wait_recv()
    sibling_waves = split(to_waves(window[2]))
    staged[...] += three(dot, (forward[2, 0], forward[2, 1]), sibling_waves)
    for load in load_back:
        load.wait()
    to_remote.wait_recv()
    to_corner_right.wait_recv()
    to_corner_left.wait_recv()
    remote_waves = split(to_waves(window[0]))
    waves = staged[...] + three(dot, (forward[0, 0], forward[0, 1]), remote_waves)

    halves = []
    for parity in range(2):
        part = waves[:, 256 * parity : 256 * parity + 256]
        mixed = cross[:, pl.ds(128 * parity, 128)]
        real_c, real_s = part[:HALF_Y, :128], part[:HALF_Y, 128:]
        imag_c, imag_s = part[HALF_Y:, :128], part[HALF_Y:, 128:]
        shift = jnp.concatenate(
            [
                jnp.concatenate([mixed * imag_s, -(mixed * imag_c)], axis=1),
                jnp.concatenate([-(mixed * real_s), mixed * real_c], axis=1),
            ],
            axis=0,
        )
        halves.append(part * even[:, pl.ds(256 * parity, 256)] + shift)
    product = split(jnp.concatenate(halves, axis=1))

    def rows_of(slot):
        return three(dot, (back[slot, 0], back[slot, 1]), product)

    low_half, high_half = pl.ds(0, HALF_X), pl.ds(HALF_X, HALF_X)
    blended[2] = rows_of(2)
    add_sibling = send(blended.at[2], from_sibling, 11, sibling)
    blended[0, :, low_half], blended[0, :, high_half] = from_waves(rows_of(0))
    add_remote = send(blended.at[0, :, centre], from_remote, 8, remote)
    add_corner_left = send(blended.at[0, :, left_strip], from_corner.at[1], 9, corner_left)
    add_corner_right = send(blended.at[0, :, right_strip], from_corner.at[0], 10, corner_right)
    blended[1] = rows_of(1)
    add_sibling.wait_recv()
    low, high = from_waves(blended[1] + from_sibling[...])
    side[0] = low[:, :MARGIN]
    add_left = send(side.at[0], from_side.at[1], 12, left)
    side[1] = high[:, MARGIN:]
    add_right = send(side.at[1], from_side.at[0], 13, right)
    middle = jnp.concatenate([low[:, MARGIN:], high[:, :MARGIN]], axis=1)
    add_remote.wait_recv()
    middle = middle + from_remote[...]
    add_corner_left.wait_recv()
    add_corner_right.wait_recv()
    middle = middle + jnp.concatenate([from_corner[0], from_corner[1]], axis=1)
    add_left.wait_recv()
    add_right.wait_recv()
    out_ref[...] = middle + jnp.concatenate([from_side[0], from_side[1]], axis=1)
    for copy in (
        to_right,
        to_left,
        to_remote,
        to_corner_right,
        to_corner_left,
        to_sibling,
        pass_left,
        pass_right,
        add_remote,
        add_corner_left,
        add_corner_right,
        add_sibling,
        add_left,
        add_right,
    ):
        copy.wait_send()


def per_device(n_ty, n_tx, noise, root_spectrum):
    forward, back, columns = tables()
    anywhere = pl.BlockSpec(memory_space=pl.ANY)
    f32 = jnp.float32
    bf16 = jnp.bfloat16
    return pl.pallas_call(
        functools.partial(kernel, n_ty, n_tx),
        out_shape=pltpu.VMEM(noise.shape, f32),
        in_specs=[anywhere] * 5,
        out_specs=pl.BlockSpec(memory_space=pltpu.VMEM),
        scratch_shapes=[
            pltpu.VMEM((3, MARGIN, EX), f32),
            pltpu.VMEM((EY, EX), f32),
            pltpu.VMEM((3, 2, EY, MARGIN), bf16),
            pltpu.VMEM((3, 2, MARGIN, EY), bf16),
            pltpu.VMEM((2, 2, HALF_X, HALF_X), bf16),
            pltpu.VMEM((EY, EX), f32),
            pltpu.VMEM((HALF_Y, HALF_X), f32),
            pltpu.VMEM((EY, EX), f32),
            pltpu.VMEM((3, MARGIN, EX), f32),
            pltpu.VMEM((2, MARGIN, MARGIN), f32),
            pltpu.VMEM((MARGIN, BLOCK), f32),
            pltpu.VMEM((MARGIN, EX), f32),
            pltpu.VMEM((2, MARGIN, MARGIN), f32),
            pltpu.VMEM((2, MARGIN, MARGIN), f32),
            pltpu.SemaphoreType.DMA((9,)),
            pltpu.SemaphoreType.DMA((14,)),
            pltpu.SemaphoreType.DMA((14,)),
        ],
        compiler_params=pltpu.CompilerParams(collective_id=0, has_side_effects=True),
        name="field_tile",
    )(noise, root_spectrum, jnp.asarray(forward), jnp.asarray(back), jnp.asarray(columns))


def solution(mesh):
    placed = (P("ty", "tx"), P())
    body = functools.partial(per_device, mesh.shape["ty"], mesh.shape["tx"])
    return jax.shard_map(
        body, mesh=mesh, in_specs=placed, out_specs=P("ty", "tx"), check_vma=False
    )
```

```python
import functools
import math

import jax
import jax.numpy as jnp
import numpy as np
from jax import lax
from jax.experimental import pallas as pl
from jax.experimental.pallas import tpu as pltpu
from jax.sharding import PartitionSpec as P

MARGIN = 128
EY = 384
EX = 512
BLOCK = 256
HALF_Y = EY // 2
HALF_X = EX // 2
MESH = pl.DeviceIdType.MESH


def split_table(table):
    high = table.astype(jnp.bfloat16)
    low = (table - high.astype(np.float64)).astype(jnp.bfloat16)
    return np.stack([high, low])


def row_basis():
    ky = np.arange(HALF_Y)[:, None]
    y = np.arange(EY)[None, :]
    angle = 2.0 * math.pi * (ky * y % EY) / EY
    lower = -np.sin(angle)
    lower[0] = np.cos(math.pi * np.arange(EY))
    return np.concatenate([np.cos(angle), lower])


def column_basis():
    x = np.arange(HALF_X)[:, None]
    bases = []
    for odd in (0, 1):
        kx = 2 * np.arange(HALF_X // 2)[None, :] + odd
        angle = 2.0 * math.pi * (kx * x % EX) / EX
        sine = np.sin(angle)
        if not odd:
            sine[:, 0] = np.cos(math.pi * np.arange(HALF_X))
        bases.append(np.concatenate([np.cos(angle), sine], axis=1))
    return np.stack(bases)


def row_weights():
    knots = (np.arange(EY) + 0.5) / MARGIN
    return np.where(
        knots < 1.0,
        0.5 * knots * knots,
        np.where(
            knots < 2.0,
            0.5 * (-2.0 * knots * knots + 6.0 * knots - 3.0),
            0.5 * (3.0 - knots) * (3.0 - knots),
        ),
    )


def tables():
    rows = row_basis()
    forward = split_table(rows)
    forward = forward.reshape(2, EY, 3, MARGIN).transpose(2, 0, 1, 3)
    back = split_table((rows * row_weights()[None, :]).T)
    back = back.reshape(2, 3, MARGIN, EY).transpose(1, 0, 2, 3)
    columns = split_table(column_basis())
    return np.ascontiguousarray(forward), np.ascontiguousarray(back), columns


def split(value):
    high = value.astype(jnp.bfloat16)
    return high, (value - high.astype(jnp.float32)).astype(jnp.bfloat16)


def dot(left, right):
    return jnp.dot(left, right, preferred_element_type=jnp.float32)


def dot_t(left, right):
    return lax.dot_general(left, right, (((1,), (1,)), ((), ())), preferred_element_type=jnp.float32)


def three(product, left, right):
    if product is dot_t:
        return dot_t(jnp.concatenate([left[0], left[1], left[0]], axis=1), jnp.concatenate([right[0], right[0], right[1]], axis=1))
    return dot(
        jnp.concatenate([left[0], left[0], left[1]], axis=1),
        jnp.concatenate([right[0], right[1], right[0]], axis=0),
    )


def iota(shape, dim):
    return lax.broadcasted_iota(jnp.int32, shape, dim)


def indicator(condition):
    return jnp.where(condition, 1.0, 0.0)


def fold_columns(spectrum):
    source = iota((EX, 128), 0)
    lane = iota((EX, 128), 1)
    folds = []
    for sign in (1.0, -1.0):
        for odd in (0, 1):
            kx = 2 * lane + odd
            fold = indicator(source == kx) + sign * indicator(source == EX - kx)
            if sign < 0 and not odd:
                fold = jnp.where(lane == 0, indicator(source == HALF_X), fold)
            folds.append(fold)
    fold = jnp.concatenate(folds, axis=1).astype(jnp.bfloat16)
    high, low = split(spectrum * (1.0 / (EY * EX)))
    return dot(high, fold) + dot(low, fold)


def fold_rows(folded, even_ref, cross_ref):
    high, low = split(folded)
    ky = iota((HALF_Y, EY), 0)
    row = iota((HALF_Y, EY), 1)
    straight = indicator(row == ky)
    mirrored = indicator(row == EY - ky)
    sums = (straight + mirrored).astype(jnp.bfloat16)
    gaps = jnp.where(ky == 0, 0.0, straight - mirrored).astype(jnp.bfloat16)
    even = dot(sums, high[:, :384]) + dot(sums, low[:, :384])
    cross = dot(gaps, high[:, 256:]) + dot(gaps, low[:, 256:])
    first_row = iota((HALF_Y, 128), 0) == 0
    first_lane = iota((HALF_Y, 128), 1) == 0
    middle = folded[HALF_Y : HALF_Y + 1]
    for slot, group in ((0, 0), (1, 0), (2, 1), (3, 1)):
        upper = even[:, 128 * group : 128 * group + 128]
        edge = jnp.broadcast_to(middle[:, 128 * group : 128 * group + 128], (HALF_Y, 128))
        if slot == 1:
            upper = jnp.where(first_lane, even[:, 256:384], upper)
            edge = jnp.where(first_lane, jnp.broadcast_to(middle[:, 256:384], (HALF_Y, 128)), edge)
        even_ref[0:HALF_Y, pl.ds(128 * slot, 128)] = upper
        even_ref[HALF_Y:EY, pl.ds(128 * slot, 128)] = jnp.where(first_row, edge, upper)
    cross_ref[:, 0:128] = jnp.where(first_lane, 0.0, cross[:, :128])
    cross_ref[:, 128:256] = cross[:, 128:]


def kernel(
    n_ty,
    n_tx,
    noise_ref,
    spectrum_ref,
    forward_ref,
    back_ref,
    columns_ref,
    out_ref,
    window,
    spectrum,
    forward,
    back,
    columns,
    even,
    cross,
    staged,
    blended,
    side,
    from_remote,
    from_sibling,
    from_side,
    from_corner,
    local_sem,
    send_sem,
    recv_sem,
):
    me_y = lax.axis_index("ty")
    me_x = lax.axis_index("tx")
    core = lax.rem(me_y, 2)
    sibling_y = me_y + 1 - 2 * core
    remote_y = lax.rem(me_y + 2 * core - 1 + n_ty, n_ty)
    left_x = lax.rem(me_x + n_tx - 1, n_tx)
    right_x = lax.rem(me_x + 1, n_tx)

    sibling = (sibling_y, me_x)
    remote = (remote_y, me_x)
    left = (me_y, left_x)
    right = (me_y, right_x)
    corner_left = (remote_y, left_x)
    corner_right = (remote_y, right_x)
    partners = (remote, corner_left, corner_right, left, right, sibling)

    barrier = pltpu.get_barrier_semaphore()
    for partner in partners:
        pl.semaphore_signal(barrier, inc=1, device_id=partner, device_id_type=MESH)

    def local(source, target, index):
        copy = pltpu.make_async_copy(source, target, local_sem.at[index])
        copy.start()
        return copy

    own = window.at[1, :, pl.ds(MARGIN, BLOCK)]
    load_noise = local(noise_ref, own, 0)
    load_spectrum = local(spectrum_ref, spectrum, 1)
    slots = (2 * core, 1, 2 - 2 * core)
    load_tables = [local(forward_ref.at[slots[i]], forward.at[i], 2 + i) for i in range(3)]
    load_columns = local(columns_ref, columns, 5)
    load_back = [local(back_ref.at[slots[i]], back.at[i], 6 + i) for i in range(3)]

    load_noise.wait()
    load_spectrum.wait()
    folded = fold_columns(spectrum[...])
    spectrum[...] = folded
    pl.semaphore_wait(barrier, len(partners))

    def send(source, target, index, device):
        copy = pltpu.make_async_remote_copy(
            src_ref=source,
            dst_ref=target,
            send_sem=send_sem.at[index],
            recv_sem=recv_sem.at[index],
            device_id=device,
            device_id_type=MESH,
        )
        copy.start()
        return copy

    left_strip = pl.ds(0, MARGIN)
    left_half = pl.ds(MARGIN, MARGIN)
    right_half = pl.ds(2 * MARGIN, MARGIN)
    right_strip = pl.ds(3 * MARGIN, MARGIN)
    centre = pl.ds(MARGIN, BLOCK)

    to_right = send(window.at[1, :, right_half], window.at[1, :, left_strip], 0, right)
    to_left = send(window.at[1, :, left_half], window.at[1, :, right_strip], 1, left)
    to_remote = send(own, window.at[0, :, centre], 2, remote)
    to_corner_right = send(window.at[1, :, right_half], window.at[0, :, left_strip], 3, corner_right)
    to_corner_left = send(window.at[1, :, left_half], window.at[0, :, right_strip], 4, corner_left)
    to_sibling = send(own, window.at[2, :, centre], 5, sibling)

    fold_rows(spectrum[...], even, cross)
    for load in load_tables:
        load.wait()
    load_columns.wait()

    def to_waves(rows):
        lower, upper = rows[:, :HALF_X], rows[:, HALF_X:]
        return jnp.concatenate(
            [
                three(dot, split(lower + upper), (columns[0, 0], columns[1, 0])),
                three(dot, split(lower - upper), (columns[0, 1], columns[1, 1])),
            ],
            axis=1,
        )

    position = iota((1, HALF_X), 1).astype(jnp.float32) + 0.5
    rising = position * (1.0 / HALF_X)
    falling = 1.0 - rising

    def from_waves(waves):
        straight = three(dot_t, split(waves[:, :HALF_X]), (columns[0, 0], columns[1, 0]))
        turned = three(dot_t, split(waves[:, HALF_X:]), (columns[0, 1], columns[1, 1]))
        return (straight + turned) * rising, (straight - turned) * falling

    to_right.wait_recv()
    pass_left = send(window.at[1, :, left_strip], window.at[2, :, left_strip], 6, sibling)
    to_left.wait_recv()
    pass_right = send(window.at[1, :, right_strip], window.at[2, :, right_strip], 7, sibling)
    own_waves = split(to_waves(window[1]))
    staged[...] = three(dot, (forward[1, 0], forward[1, 1]), own_waves)
    to_sibling.wait_recv()
    pass_left.wait_recv()
    pass_right.wait_recv()
    sibling_waves = split(to_waves(window[2]))
    staged[...] += three(dot, (forward[2, 0], forward[2, 1]), sibling_waves)
    for load in load_back:
        load.wait()
    to_remote.wait_recv()
    to_corner_right.wait_recv()
    to_corner_left.wait_recv()
    remote_waves = split(to_waves(window[0]))
    waves = staged[...] + three(dot, (forward[0, 0], forward[0, 1]), remote_waves)

    halves = []
    for parity in range(2):
        part = waves[:, 256 * parity : 256 * parity + 256]
        mixed = cross[:, pl.ds(128 * parity, 128)]
        real_c, real_s = part[:HALF_Y, :128], part[:HALF_Y, 128:]
        imag_c, imag_s = part[HALF_Y:, :128], part[HALF_Y:, 128:]
        shift = jnp.concatenate(
            [
                jnp.concatenate([mixed * imag_s, -(mixed * imag_c)], axis=1),
                jnp.concatenate([-(mixed * real_s), mixed * real_c], axis=1),
            ],
            axis=0,
        )
        halves.append(part * even[:, pl.ds(256 * parity, 256)] + shift)
    product = split(jnp.concatenate(halves, axis=1))

    def rows_of(slot):
        return three(dot, (back[slot, 0], back[slot, 1]), product)

    low_half, high_half = pl.ds(0, HALF_X), pl.ds(HALF_X, HALF_X)
    blended[2] = rows_of(2)
    add_sibling = send(blended.at[2], from_sibling, 11, sibling)
    blended[0, :, low_half], blended[0, :, high_half] = from_waves(rows_of(0))
    add_remote = send(blended.at[0, :, centre], from_remote, 8, remote)
    add_corner_left = send(blended.at[0, :, left_strip], from_corner.at[1], 9, corner_left)
    add_corner_right = send(blended.at[0, :, right_strip], from_corner.at[0], 10, corner_right)
    blended[1] = rows_of(1)
    add_sibling.wait_recv()
    low, high = from_waves(blended[1] + from_sibling[...])
    side[0] = low[:, :MARGIN]
    add_left = send(side.at[0], from_side.at[1], 12, left)
    side[1] = high[:, MARGIN:]
    add_right = send(side.at[1], from_side.at[0], 13, right)
    middle = jnp.concatenate([low[:, MARGIN:], high[:, :MARGIN]], axis=1)
    add_remote.wait_recv()
    middle = middle + from_remote[...]
    add_corner_left.wait_recv()
    add_corner_right.wait_recv()
    middle = middle + jnp.concatenate([from_corner[0], from_corner[1]], axis=1)
    add_left.wait_recv()
    add_right.wait_recv()
    out_ref[...] = middle + jnp.concatenate([from_side[0], from_side[1]], axis=1)
    for copy in (
        to_right,
        to_left,
        to_remote,
        to_corner_right,
        to_corner_left,
        to_sibling,
        pass_left,
        pass_right,
        add_remote,
        add_corner_left,
        add_corner_right,
        add_sibling,
        add_left,
        add_right,
    ):
        copy.wait_send()


def per_device(n_ty, n_tx, noise, root_spectrum):
    forward, back, columns = tables()
    anywhere = pl.BlockSpec(memory_space=pl.ANY)
    f32 = jnp.float32
    bf16 = jnp.bfloat16
    return pl.pallas_call(
        functools.partial(kernel, n_ty, n_tx),
        out_shape=pltpu.VMEM(noise.shape, f32),
        in_specs=[anywhere] * 5,
        out_specs=pl.BlockSpec(memory_space=pltpu.VMEM),
        scratch_shapes=[
            pltpu.VMEM((3, MARGIN, EX), f32),
            pltpu.VMEM((EY, EX), f32),
            pltpu.VMEM((3, 2, EY, MARGIN), bf16),
            pltpu.VMEM((3, 2, MARGIN, EY), bf16),
            pltpu.VMEM((2, 2, HALF_X, HALF_X), bf16),
            pltpu.VMEM((EY, EX), f32),
            pltpu.VMEM((HALF_Y, HALF_X), f32),
            pltpu.VMEM((EY, EX), f32),
            pltpu.VMEM((3, MARGIN, EX), f32),
            pltpu.VMEM((2, MARGIN, MARGIN), f32),
            pltpu.VMEM((MARGIN, BLOCK), f32),
            pltpu.VMEM((MARGIN, EX), f32),
            pltpu.VMEM((2, MARGIN, MARGIN), f32),
            pltpu.VMEM((2, MARGIN, MARGIN), f32),
            pltpu.SemaphoreType.DMA((9,)),
            pltpu.SemaphoreType.DMA((14,)),
            pltpu.SemaphoreType.DMA((14,)),
        ],
        compiler_params=pltpu.CompilerParams(collective_id=0, has_side_effects=True),
        name="field_tile",
    )(noise, root_spectrum, jnp.asarray(forward), jnp.asarray(back), jnp.asarray(columns))


def solution(mesh):
    placed = (P("ty", "tx"), P())
    body = functools.partial(per_device, mesh.shape["ty"], mesh.shape["tx"])
    return jax.shard_map(
        body, mesh=mesh, in_specs=placed, out_specs=P("ty", "tx"), check_vma=False
    )
```

```python
import functools
import math

import jax
import jax.numpy as jnp
import numpy as np
from jax import lax
from jax.experimental import pallas as pl
from jax.experimental.pallas import tpu as pltpu
from jax.sharding import PartitionSpec as P

MARGIN = 128
EY = 384
EX = 512
BLOCK = 256
HALF_Y = EY // 2
HALF_X = EX // 2
MESH = pl.DeviceIdType.MESH


def split_table(table):
    high = table.astype(jnp.bfloat16)
    low = (table - high.astype(np.float64)).astype(jnp.bfloat16)
    return np.stack([high, low])


def row_basis():
    ky = np.arange(HALF_Y)[:, None]
    y = np.arange(EY)[None, :]
    angle = 2.0 * math.pi * (ky * y % EY) / EY
    lower = -np.sin(angle)
    lower[0] = np.cos(math.pi * np.arange(EY))
    return np.concatenate([np.cos(angle), lower])


def column_basis():
    x = np.arange(HALF_X)[:, None]
    bases = []
    for odd in (0, 1):
        kx = 2 * np.arange(HALF_X // 2)[None, :] + odd
        angle = 2.0 * math.pi * (kx * x % EX) / EX
        sine = np.sin(angle)
        if not odd:
            sine[:, 0] = np.cos(math.pi * np.arange(HALF_X))
        bases.append(np.concatenate([np.cos(angle), sine], axis=1))
    return np.stack(bases)


def row_weights():
    knots = (np.arange(EY) + 0.5) / MARGIN
    return np.where(
        knots < 1.0,
        0.5 * knots * knots,
        np.where(
            knots < 2.0,
            0.5 * (-2.0 * knots * knots + 6.0 * knots - 3.0),
            0.5 * (3.0 - knots) * (3.0 - knots),
        ),
    )


def tables():
    rows = row_basis()
    forward = split_table(rows)
    forward = forward.reshape(2, EY, 3, MARGIN).transpose(2, 0, 1, 3)
    back = split_table((rows * row_weights()[None, :]).T)
    back = back.reshape(2, 3, MARGIN, EY).transpose(1, 0, 2, 3)
    columns = split_table(column_basis())
    turned = columns.transpose(0, 1, 3, 2)
    return [np.ascontiguousarray(table) for table in (forward, back, columns, turned)]


def split(value):
    high = value.astype(jnp.bfloat16)
    return high, (value - high.astype(jnp.float32)).astype(jnp.bfloat16)


def dot(left, right):
    return jnp.dot(left, right, preferred_element_type=jnp.float32)


def three(left, right):
    return dot(
        jnp.concatenate([left[0], left[0], left[1]], axis=1),
        jnp.concatenate([right[0], right[1], right[0]], axis=0),
    )


def iota(shape, dim):
    return lax.broadcasted_iota(jnp.int32, shape, dim)


def indicator(condition):
    return jnp.where(condition, 1.0, 0.0)


def fold_columns(spectrum):
    source = iota((EX, 128), 0)
    lane = iota((EX, 128), 1)
    folds = []
    for sign in (1.0, -1.0):
        for odd in (0, 1):
            kx = 2 * lane + odd
            fold = indicator(source == kx) + sign * indicator(source == EX - kx)
            if sign < 0 and not odd:
                fold = jnp.where(lane == 0, indicator(source == HALF_X), fold)
            folds.append(fold)
    fold = jnp.concatenate(folds, axis=1).astype(jnp.bfloat16)
    high, low = split(spectrum * (1.0 / (EY * EX)))
    return dot(high, fold) + dot(low, fold)


def fold_rows(folded, even_ref, cross_ref):
    high, low = split(folded)
    ky = iota((HALF_Y, EY), 0)
    row = iota((HALF_Y, EY), 1)
    straight = indicator(row == ky)
    mirrored = indicator(row == EY - ky)
    sums = (straight + mirrored).astype(jnp.bfloat16)
    gaps = jnp.where(ky == 0, 0.0, straight - mirrored).astype(jnp.bfloat16)
    even = dot(sums, high[:, :384]) + dot(sums, low[:, :384])
    cross = dot(gaps, high[:, 256:]) + dot(gaps, low[:, 256:])
    first_row = iota((HALF_Y, 128), 0) == 0
    first_lane = iota((HALF_Y, 128), 1) == 0
    middle = folded[HALF_Y : HALF_Y + 1]
    for slot, group in ((0, 0), (1, 0), (2, 1), (3, 1)):
        upper = even[:, 128 * group : 128 * group + 128]
        edge = jnp.broadcast_to(middle[:, 128 * group : 128 * group + 128], (HALF_Y, 128))
        if slot == 1:
            upper = jnp.where(first_lane, even[:, 256:384], upper)
            edge = jnp.where(first_lane, jnp.broadcast_to(middle[:, 256:384], (HALF_Y, 128)), edge)
        even_ref[0:HALF_Y, pl.ds(128 * slot, 128)] = upper
        even_ref[HALF_Y:EY, pl.ds(128 * slot, 128)] = jnp.where(first_row, edge, upper)
    cross_ref[:, 0:128] = jnp.where(first_lane, 0.0, cross[:, :128])
    cross_ref[:, 128:256] = cross[:, 128:]


def kernel(
    n_ty,
    n_tx,
    noise_ref,
    spectrum_ref,
    forward_ref,
    back_ref,
    columns_ref,
    turned_ref,
    out_ref,
    window,
    spectrum,
    forward,
    back,
    columns,
    turned,
    even,
    cross,
    staged,
    blended,
    side,
    from_remote,
    from_sibling,
    from_side,
    from_corner,
    local_sem,
    send_sem,
    recv_sem,
):
    me_y = lax.axis_index("ty")
    me_x = lax.axis_index("tx")
    core = lax.rem(me_y, 2)
    sibling_y = me_y + 1 - 2 * core
    remote_y = lax.rem(me_y + 2 * core - 1 + n_ty, n_ty)
    left_x = lax.rem(me_x + n_tx - 1, n_tx)
    right_x = lax.rem(me_x + 1, n_tx)

    sibling = (sibling_y, me_x)
    remote = (remote_y, me_x)
    left = (me_y, left_x)
    right = (me_y, right_x)
    corner_left = (remote_y, left_x)
    corner_right = (remote_y, right_x)
    partners = (remote, corner_left, corner_right, left, right, sibling)

    barrier = pltpu.get_barrier_semaphore()
    for partner in partners:
        pl.semaphore_signal(barrier, inc=1, device_id=partner, device_id_type=MESH)

    def local(source, target, index):
        copy = pltpu.make_async_copy(source, target, local_sem.at[index])
        copy.start()
        return copy

    own = window.at[1, :, pl.ds(MARGIN, BLOCK)]
    load_noise = local(noise_ref, own, 0)
    load_spectrum = local(spectrum_ref, spectrum, 1)
    slots = (2 * core, 1, 2 - 2 * core)
    load_tables = [local(forward_ref.at[slots[i]], forward.at[i], 2 + i) for i in range(3)]
    load_columns = local(columns_ref, columns, 5)
    load_turned = local(turned_ref, turned, 9)
    load_back = [local(back_ref.at[slots[i]], back.at[i], 6 + i) for i in range(3)]

    load_noise.wait()
    load_spectrum.wait()
    folded = fold_columns(spectrum[...])
    spectrum[...] = folded
    pl.semaphore_wait(barrier, len(partners))

    def send(source, target, index, device):
        copy = pltpu.make_async_remote_copy(
            src_ref=source,
            dst_ref=target,
            send_sem=send_sem.at[index],
            recv_sem=recv_sem.at[index],
            device_id=device,
            device_id_type=MESH,
        )
        copy.start()
        return copy

    left_strip = pl.ds(0, MARGIN)
    left_half = pl.ds(MARGIN, MARGIN)
    right_half = pl.ds(2 * MARGIN, MARGIN)
    right_strip = pl.ds(3 * MARGIN, MARGIN)
    centre = pl.ds(MARGIN, BLOCK)

    to_right = send(window.at[1, :, right_half], window.at[1, :, left_strip], 0, right)
    to_left = send(window.at[1, :, left_half], window.at[1, :, right_strip], 1, left)
    to_corner_left = send(window.at[1, :, left_half], window.at[0, :, right_strip], 4, corner_left)
    to_remote = send(own, window.at[0, :, centre], 2, remote)
    to_corner_right = send(window.at[1, :, right_half], window.at[0, :, left_strip], 3, corner_right)
    to_sibling = send(own, window.at[2, :, centre], 5, sibling)

    fold_rows(spectrum[...], even, cross)
    for load in load_tables:
        load.wait()
    load_columns.wait()

    def to_waves(rows):
        lower, upper = rows[:, :HALF_X], rows[:, HALF_X:]
        return jnp.concatenate(
            [
                three(split(lower + upper), (columns[0, 0], columns[1, 0])),
                three(split(lower - upper), (columns[0, 1], columns[1, 1])),
            ],
            axis=1,
        )

    position = iota((1, HALF_X), 1).astype(jnp.float32) + 0.5
    rising = position * (1.0 / HALF_X)
    falling = 1.0 - rising

    def from_waves(waves):
        straight = three(split(waves[:, :HALF_X]), (turned[0, 0], turned[1, 0]))
        crossed = three(split(waves[:, HALF_X:]), (turned[0, 1], turned[1, 1]))
        return (straight + crossed) * rising, (straight - crossed) * falling

    to_right.wait_recv()
    pass_left = send(window.at[1, :, left_strip], window.at[2, :, left_strip], 6, sibling)
    to_left.wait_recv()
    pass_right = send(window.at[1, :, right_strip], window.at[2, :, right_strip], 7, sibling)
    own_waves = split(to_waves(window[1]))
    staged[...] = three((forward[1, 0], forward[1, 1]), own_waves)
    to_sibling.wait_recv()
    pass_left.wait_recv()
    pass_right.wait_recv()
    sibling_waves = split(to_waves(window[2]))
    staged[...] += three((forward[2, 0], forward[2, 1]), sibling_waves)
    for load in (*load_back, load_turned):
        load.wait()
    to_remote.wait_recv()
    to_corner_right.wait_recv()
    to_corner_left.wait_recv()
    remote_waves = split(to_waves(window[0]))
    waves = staged[...] + three((forward[0, 0], forward[0, 1]), remote_waves)

    halves = []
    for parity in range(2):
        part = waves[:, 256 * parity : 256 * parity + 256]
        mixed = cross[:, pl.ds(128 * parity, 128)]
        real_c, real_s = part[:HALF_Y, :128], part[:HALF_Y, 128:]
        imag_c, imag_s = part[HALF_Y:, :128], part[HALF_Y:, 128:]
        shift = jnp.concatenate(
            [
                jnp.concatenate([mixed * imag_s, -(mixed * imag_c)], axis=1),
                jnp.concatenate([-(mixed * real_s), mixed * real_c], axis=1),
            ],
            axis=0,
        )
        halves.append(part * even[:, pl.ds(256 * parity, 256)] + shift)
    product = split(jnp.concatenate(halves, axis=1))

    def rows_of(slot):
        return three((back[slot, 0], back[slot, 1]), product)

    low_half, high_half = pl.ds(0, HALF_X), pl.ds(HALF_X, HALF_X)
    blended[2] = rows_of(2)
    add_sibling = send(blended.at[2], from_sibling, 11, sibling)
    blended[0, :, low_half], blended[0, :, high_half] = from_waves(rows_of(0))
    add_remote = send(blended.at[0, :, centre], from_remote, 8, remote)
    add_corner_left = send(blended.at[0, :, left_strip], from_corner.at[1], 9, corner_left)
    add_corner_right = send(blended.at[0, :, right_strip], from_corner.at[0], 10, corner_right)
    blended[1] = rows_of(1)
    add_sibling.wait_recv()
    low, high = from_waves(blended[1] + from_sibling[...])
    side[0] = low[:, :MARGIN]
    add_left = send(side.at[0], from_side.at[1], 12, left)
    side[1] = high[:, MARGIN:]
    add_right = send(side.at[1], from_side.at[0], 13, right)
    middle = jnp.concatenate([low[:, MARGIN:], high[:, :MARGIN]], axis=1)
    add_remote.wait_recv()
    middle = middle + from_remote[...]
    add_corner_left.wait_recv()
    add_corner_right.wait_recv()
    middle = middle + jnp.concatenate([from_corner[0], from_corner[1]], axis=1)
    add_left.wait_recv()
    add_right.wait_recv()
    out_ref[...] = middle + jnp.concatenate([from_side[0], from_side[1]], axis=1)
    for copy in (
        to_right,
        to_left,
        to_remote,
        to_corner_right,
        to_corner_left,
        to_sibling,
        pass_left,
        pass_right,
        add_remote,
        add_corner_left,
        add_corner_right,
        add_sibling,
        add_left,
        add_right,
    ):
        copy.wait_send()


def per_device(n_ty, n_tx, noise, root_spectrum):
    constants = [jnp.asarray(table) for table in tables()]
    anywhere = pl.BlockSpec(memory_space=pl.ANY)
    f32 = jnp.float32
    bf16 = jnp.bfloat16
    return pl.pallas_call(
        functools.partial(kernel, n_ty, n_tx),
        out_shape=pltpu.VMEM(noise.shape, f32),
        in_specs=[anywhere] * 6,
        out_specs=pl.BlockSpec(memory_space=pltpu.VMEM),
        scratch_shapes=[
            pltpu.VMEM((3, MARGIN, EX), f32),
            pltpu.VMEM((EY, EX), f32),
            pltpu.VMEM((3, 2, EY, MARGIN), bf16),
            pltpu.VMEM((3, 2, MARGIN, EY), bf16),
            pltpu.VMEM((2, 2, HALF_X, HALF_X), bf16),
            pltpu.VMEM((2, 2, HALF_X, HALF_X), bf16),
            pltpu.VMEM((EY, EX), f32),
            pltpu.VMEM((HALF_Y, HALF_X), f32),
            pltpu.VMEM((EY, EX), f32),
            pltpu.VMEM((3, MARGIN, EX), f32),
            pltpu.VMEM((2, MARGIN, MARGIN), f32),
            pltpu.VMEM((MARGIN, BLOCK), f32),
            pltpu.VMEM((MARGIN, EX), f32),
            pltpu.VMEM((2, MARGIN, MARGIN), f32),
            pltpu.VMEM((2, MARGIN, MARGIN), f32),
            pltpu.SemaphoreType.DMA((10,)),
            pltpu.SemaphoreType.DMA((14,)),
            pltpu.SemaphoreType.DMA((14,)),
        ],
        compiler_params=pltpu.CompilerParams(collective_id=0, has_side_effects=True),
        name="field_tile",
    )(noise, root_spectrum, *constants)


def solution(mesh):
    placed = (P("ty", "tx"), P())
    body = functools.partial(per_device, mesh.shape["ty"], mesh.shape["tx"])
    return jax.shard_map(
        body, mesh=mesh, in_specs=placed, out_specs=P("ty", "tx"), check_vma=False
    )
```

```python
import functools
import math

import jax
import jax.numpy as jnp
import numpy as np
from jax import lax
from jax.experimental import pallas as pl
from jax.experimental.pallas import tpu as pltpu
from jax.sharding import PartitionSpec as P

MARGIN = 128
EY = 384
EX = 512
BLOCK = 256
HALF_Y = EY // 2
HALF_X = EX // 2
MESH = pl.DeviceIdType.MESH


def split_table(table):
    high = table.astype(jnp.bfloat16)
    low = (table - high.astype(np.float64)).astype(jnp.bfloat16)
    return np.stack([high, low])


def row_basis():
    ky = np.arange(HALF_Y)[:, None]
    y = np.arange(EY)[None, :]
    angle = 2.0 * math.pi * (ky * y % EY) / EY
    lower = -np.sin(angle)
    lower[0] = np.cos(math.pi * np.arange(EY))
    return np.concatenate([np.cos(angle), lower])


def column_basis():
    x = np.arange(HALF_X)[:, None]
    bases = []
    for odd in (0, 1):
        kx = 2 * np.arange(HALF_X // 2)[None, :] + odd
        angle = 2.0 * math.pi * (kx * x % EX) / EX
        sine = np.sin(angle)
        if not odd:
            sine[:, 0] = np.cos(math.pi * np.arange(HALF_X))
        bases.append(np.concatenate([np.cos(angle), sine], axis=1))
    return np.stack(bases)


def row_weights():
    knots = (np.arange(EY) + 0.5) / MARGIN
    return np.where(
        knots < 1.0,
        0.5 * knots * knots,
        np.where(
            knots < 2.0,
            0.5 * (-2.0 * knots * knots + 6.0 * knots - 3.0),
            0.5 * (3.0 - knots) * (3.0 - knots),
        ),
    )


def tables():
    rows = row_basis()
    forward = split_table(rows)
    forward = forward.reshape(2, EY, 3, MARGIN).transpose(2, 0, 1, 3)
    back = split_table((rows * row_weights()[None, :]).T)
    back = back.reshape(2, 3, MARGIN, EY).transpose(1, 0, 2, 3)
    columns = split_table(column_basis())
    turned = columns.transpose(0, 1, 3, 2)
    return [np.ascontiguousarray(table) for table in (forward, back, columns, turned)]


def split(value):
    high = value.astype(jnp.bfloat16)
    return high, (value - high.astype(jnp.float32)).astype(jnp.bfloat16)


def dot(left, right):
    return jnp.dot(left, right, preferred_element_type=jnp.float32)


def three(left, right):
    return dot(
        jnp.concatenate([left[0], left[0], left[1]], axis=1),
        jnp.concatenate([right[0], right[1], right[0]], axis=0),
    )


def iota(shape, dim):
    return lax.broadcasted_iota(jnp.int32, shape, dim)


def indicator(condition):
    return jnp.where(condition, 1.0, 0.0)


def fold_columns(spectrum):
    source = iota((EX, 128), 0)
    lane = iota((EX, 128), 1)
    folds = []
    for sign in (1.0, -1.0):
        for odd in (0, 1):
            kx = 2 * lane + odd
            fold = indicator(source == kx) + sign * indicator(source == EX - kx)
            if sign < 0 and not odd:
                fold = jnp.where(lane == 0, indicator(source == HALF_X), fold)
            folds.append(fold)
    fold = jnp.concatenate(folds, axis=1).astype(jnp.bfloat16)
    high, low = split(spectrum * (1.0 / (EY * EX)))
    return dot(high, fold) + dot(low, fold)


def fold_rows(folded, even_ref, cross_ref):
    high, low = split(folded)
    ky = iota((HALF_Y, EY), 0)
    row = iota((HALF_Y, EY), 1)
    straight = indicator(row == ky)
    mirrored = indicator(row == EY - ky)
    sums = (straight + mirrored).astype(jnp.bfloat16)
    gaps = jnp.where(ky == 0, 0.0, straight - mirrored).astype(jnp.bfloat16)
    even = dot(sums, high[:, :384]) + dot(sums, low[:, :384])
    cross = dot(gaps, high[:, 256:]) + dot(gaps, low[:, 256:])
    first_row = iota((HALF_Y, 128), 0) == 0
    first_lane = iota((HALF_Y, 128), 1) == 0
    middle = folded[HALF_Y : HALF_Y + 1]
    for slot, group in ((0, 0), (1, 0), (2, 1), (3, 1)):
        upper = even[:, 128 * group : 128 * group + 128]
        edge = jnp.broadcast_to(middle[:, 128 * group : 128 * group + 128], (HALF_Y, 128))
        if slot == 1:
            upper = jnp.where(first_lane, even[:, 256:384], upper)
            edge = jnp.where(first_lane, jnp.broadcast_to(middle[:, 256:384], (HALF_Y, 128)), edge)
        even_ref[0:HALF_Y, pl.ds(128 * slot, 128)] = upper
        even_ref[HALF_Y:EY, pl.ds(128 * slot, 128)] = jnp.where(first_row, edge, upper)
    cross_ref[:, 0:128] = jnp.where(first_lane, 0.0, cross[:, :128])
    cross_ref[:, 128:256] = cross[:, 128:]


def kernel(
    n_ty,
    n_tx,
    noise_ref,
    spectrum_ref,
    forward_ref,
    back_ref,
    columns_ref,
    turned_ref,
    out_ref,
    window,
    spectrum,
    forward,
    back,
    columns,
    turned,
    even,
    cross,
    staged,
    blended,
    side,
    from_remote,
    from_sibling,
    from_side,
    from_corner,
    local_sem,
    send_sem,
    recv_sem,
):
    me_y = lax.axis_index("ty")
    me_x = lax.axis_index("tx")
    core = lax.rem(me_y, 2)
    sibling_y = me_y + 1 - 2 * core
    remote_y = lax.rem(me_y + 2 * core - 1 + n_ty, n_ty)
    left_x = lax.rem(me_x + n_tx - 1, n_tx)
    right_x = lax.rem(me_x + 1, n_tx)

    sibling = (sibling_y, me_x)
    remote = (remote_y, me_x)
    left = (me_y, left_x)
    right = (me_y, right_x)
    corner_left = (remote_y, left_x)
    corner_right = (remote_y, right_x)
    partners = (remote, corner_left, corner_right, left, right, sibling)

    barrier = pltpu.get_barrier_semaphore()
    for partner in partners:
        pl.semaphore_signal(barrier, inc=1, device_id=partner, device_id_type=MESH)

    def local(source, target, index):
        copy = pltpu.make_async_copy(source, target, local_sem.at[index])
        copy.start()
        return copy

    own = window.at[1, :, pl.ds(MARGIN, BLOCK)]
    load_noise = local(noise_ref, own, 0)
    load_spectrum = local(spectrum_ref, spectrum, 1)
    slots = (2 * core, 1, 2 - 2 * core)
    load_tables = [local(forward_ref.at[slots[i]], forward.at[i], 2 + i) for i in range(3)]
    load_columns = local(columns_ref, columns, 5)
    load_turned = local(turned_ref, turned, 9)
    load_back = [local(back_ref.at[slots[i]], back.at[i], 6 + i) for i in range(3)]

    load_noise.wait()
    load_spectrum.wait()
    folded = fold_columns(spectrum[...])
    spectrum[...] = folded
    pl.semaphore_wait(barrier, len(partners))

    def send(source, target, index, device):
        copy = pltpu.make_async_remote_copy(
            src_ref=source,
            dst_ref=target,
            send_sem=send_sem.at[index],
            recv_sem=recv_sem.at[index],
            device_id=device,
            device_id_type=MESH,
        )
        copy.start()
        return copy

    left_strip = pl.ds(0, MARGIN)
    left_half = pl.ds(MARGIN, MARGIN)
    right_half = pl.ds(2 * MARGIN, MARGIN)
    right_strip = pl.ds(3 * MARGIN, MARGIN)
    centre = pl.ds(MARGIN, BLOCK)

    to_right = send(window.at[1, :, right_half], window.at[1, :, left_strip], 0, right)
    to_left = send(window.at[1, :, left_half], window.at[1, :, right_strip], 1, left)
    to_corner_left = send(window.at[1, :, left_half], window.at[0, :, right_strip], 4, corner_left)
    to_remote = send(own, window.at[0, :, centre], 2, remote)
    to_corner_right = send(window.at[1, :, right_half], window.at[0, :, left_strip], 3, corner_right)
    to_sibling = send(own, window.at[2, :, centre], 5, sibling)

    fold_rows(spectrum[...], even, cross)
    for load in load_tables:
        load.wait()
    load_columns.wait()

    def to_waves(rows):
        lower, upper = rows[:, :HALF_X], rows[:, HALF_X:]
        return jnp.concatenate(
            [
                three(split(lower + upper), (columns[0, 0], columns[1, 0])),
                three(split(lower - upper), (columns[0, 1], columns[1, 1])),
            ],
            axis=1,
        )

    position = iota((1, HALF_X), 1).astype(jnp.float32) + 0.5
    rising = position * (1.0 / HALF_X)
    falling = 1.0 - rising

    def from_waves(waves):
        straight = three(split(waves[:, :HALF_X]), (turned[0, 0], turned[1, 0]))
        crossed = three(split(waves[:, HALF_X:]), (turned[0, 1], turned[1, 1]))
        return (straight + crossed) * rising, (straight - crossed) * falling

    to_right.wait_recv()
    pass_left = send(window.at[1, :, left_strip], window.at[2, :, left_strip], 6, sibling)
    to_left.wait_recv()
    pass_right = send(window.at[1, :, right_strip], window.at[2, :, right_strip], 7, sibling)
    own_waves = split(to_waves(window[1]))
    staged[...] = three((forward[1, 0], forward[1, 1]), own_waves)
    to_sibling.wait_recv()
    pass_left.wait_recv()
    pass_right.wait_recv()
    sibling_waves = split(to_waves(window[2]))
    for load in (*load_back, load_turned):
        load.wait()
    to_remote.wait_recv()
    to_corner_right.wait_recv()
    to_corner_left.wait_recv()
    remote_waves = split(to_waves(window[0]))
    pairs = ((forward[2, 0], forward[2, 1], sibling_waves), (forward[0, 0], forward[0, 1], remote_waves))
    waves = staged[...] + dot(
        jnp.concatenate([t for high, low, _ in pairs for t in (high, high, low)], axis=1),
        jnp.concatenate([w for _, _, (high, low) in pairs for w in (high, low, high)], axis=0),
    )

    halves = []
    for parity in range(2):
        part = waves[:, 256 * parity : 256 * parity + 256]
        mixed = cross[:, pl.ds(128 * parity, 128)]
        real_c, real_s = part[:HALF_Y, :128], part[:HALF_Y, 128:]
        imag_c, imag_s = part[HALF_Y:, :128], part[HALF_Y:, 128:]
        shift = jnp.concatenate(
            [
                jnp.concatenate([mixed * imag_s, -(mixed * imag_c)], axis=1),
                jnp.concatenate([-(mixed * real_s), mixed * real_c], axis=1),
            ],
            axis=0,
        )
        halves.append(part * even[:, pl.ds(256 * parity, 256)] + shift)
    product = split(jnp.concatenate(halves, axis=1))

    def rows_of(slot):
        return three((back[slot, 0], back[slot, 1]), product)

    low_half, high_half = pl.ds(0, HALF_X), pl.ds(HALF_X, HALF_X)
    blended[0, :, low_half], blended[0, :, high_half] = from_waves(rows_of(0))
    add_remote = send(blended.at[0, :, centre], from_remote, 8, remote)
    add_corner_left = send(blended.at[0, :, left_strip], from_corner.at[1], 9, corner_left)
    add_corner_right = send(blended.at[0, :, right_strip], from_corner.at[0], 10, corner_right)
    blended[2] = rows_of(2)
    add_sibling = send(blended.at[2], from_sibling, 11, sibling)
    blended[1] = rows_of(1)
    add_sibling.wait_recv()
    low, high = from_waves(blended[1] + from_sibling[...])
    side[0] = low[:, :MARGIN]
    add_left = send(side.at[0], from_side.at[1], 12, left)
    side[1] = high[:, MARGIN:]
    add_right = send(side.at[1], from_side.at[0], 13, right)
    middle = jnp.concatenate([low[:, MARGIN:], high[:, :MARGIN]], axis=1)
    add_remote.wait_recv()
    middle = middle + from_remote[...]
    add_corner_left.wait_recv()
    add_corner_right.wait_recv()
    middle = middle + jnp.concatenate([from_corner[0], from_corner[1]], axis=1)
    add_left.wait_recv()
    add_right.wait_recv()
    out_ref[...] = middle + jnp.concatenate([from_side[0], from_side[1]], axis=1)
    for copy in (
        to_right,
        to_left,
        to_remote,
        to_corner_right,
        to_corner_left,
        to_sibling,
        pass_left,
        pass_right,
        add_remote,
        add_corner_left,
        add_corner_right,
        add_sibling,
        add_left,
        add_right,
    ):
        copy.wait_send()


def per_device(n_ty, n_tx, noise, root_spectrum):
    constants = [jnp.asarray(table) for table in tables()]
    anywhere = pl.BlockSpec(memory_space=pl.ANY)
    f32 = jnp.float32
    bf16 = jnp.bfloat16
    return pl.pallas_call(
        functools.partial(kernel, n_ty, n_tx),
        out_shape=pltpu.VMEM(noise.shape, f32),
        in_specs=[anywhere] * 6,
        out_specs=pl.BlockSpec(memory_space=pltpu.VMEM),
        scratch_shapes=[
            pltpu.VMEM((3, MARGIN, EX), f32),
            pltpu.VMEM((EY, EX), f32),
            pltpu.VMEM((3, 2, EY, MARGIN), bf16),
            pltpu.VMEM((3, 2, MARGIN, EY), bf16),
            pltpu.VMEM((2, 2, HALF_X, HALF_X), bf16),
            pltpu.VMEM((2, 2, HALF_X, HALF_X), bf16),
            pltpu.VMEM((EY, EX), f32),
            pltpu.VMEM((HALF_Y, HALF_X), f32),
            pltpu.VMEM((EY, EX), f32),
            pltpu.VMEM((3, MARGIN, EX), f32),
            pltpu.VMEM((2, MARGIN, MARGIN), f32),
            pltpu.VMEM((MARGIN, BLOCK), f32),
            pltpu.VMEM((MARGIN, EX), f32),
            pltpu.VMEM((2, MARGIN, MARGIN), f32),
            pltpu.VMEM((2, MARGIN, MARGIN), f32),
            pltpu.SemaphoreType.DMA((10,)),
            pltpu.SemaphoreType.DMA((14,)),
            pltpu.SemaphoreType.DMA((14,)),
        ],
        compiler_params=pltpu.CompilerParams(collective_id=0, has_side_effects=True),
        name="field_tile",
    )(noise, root_spectrum, *constants)


def solution(mesh):
    placed = (P("ty", "tx"), P())
    body = functools.partial(per_device, mesh.shape["ty"], mesh.shape["tx"])
    return jax.shard_map(
        body, mesh=mesh, in_specs=placed, out_specs=P("ty", "tx"), check_vma=False
    )
```

```python
import functools
import math

import jax
import jax.numpy as jnp
import numpy as np
from jax import lax
from jax.experimental import pallas as pl
from jax.experimental.pallas import tpu as pltpu
from jax.sharding import PartitionSpec as P

MARGIN = 128
EY = 384
EX = 512
BLOCK = 256
HALF_Y = EY // 2
HALF_X = EX // 2
MESH = pl.DeviceIdType.MESH


def split_table(table):
    high = table.astype(jnp.bfloat16)
    low = (table - high.astype(np.float64)).astype(jnp.bfloat16)
    return np.stack([high, low])


def row_basis():
    ky = np.arange(HALF_Y)[:, None]
    y = np.arange(EY)[None, :]
    angle = 2.0 * math.pi * (ky * y % EY) / EY
    lower = -np.sin(angle)
    lower[0] = np.cos(math.pi * np.arange(EY))
    return np.concatenate([np.cos(angle), lower])


def column_basis():
    x = np.arange(HALF_X)[:, None]
    bases = []
    for odd in (0, 1):
        kx = 2 * np.arange(HALF_X // 2)[None, :] + odd
        angle = 2.0 * math.pi * (kx * x % EX) / EX
        sine = np.sin(angle)
        if not odd:
            sine[:, 0] = np.cos(math.pi * np.arange(HALF_X))
        bases.append(np.concatenate([np.cos(angle), sine], axis=1))
    return np.stack(bases)


def row_weights():
    knots = (np.arange(EY) + 0.5) / MARGIN
    return np.where(
        knots < 1.0,
        0.5 * knots * knots,
        np.where(
            knots < 2.0,
            0.5 * (-2.0 * knots * knots + 6.0 * knots - 3.0),
            0.5 * (3.0 - knots) * (3.0 - knots),
        ),
    )


def tables():
    rows = row_basis()
    forward = split_table(rows)
    forward = forward.reshape(2, EY, 3, MARGIN).transpose(2, 0, 1, 3)
    back = split_table((rows * row_weights()[None, :]).T)
    back = back.reshape(2, 3, MARGIN, EY).transpose(1, 0, 2, 3)
    columns = split_table(column_basis())
    turned = columns.transpose(0, 1, 3, 2)
    return [np.ascontiguousarray(table) for table in (forward, back, columns, turned)]


def split(value):
    high = value.astype(jnp.bfloat16)
    return high, (value - high.astype(jnp.float32)).astype(jnp.bfloat16)


def dot(left, right):
    return jnp.dot(left, right, preferred_element_type=jnp.float32)


def three(left, right):
    return dot(
        jnp.concatenate([left[0], left[0], left[1]], axis=1),
        jnp.concatenate([right[0], right[1], right[0]], axis=0),
    )


def iota(shape, dim):
    return lax.broadcasted_iota(jnp.int32, shape, dim)


def indicator(condition):
    return jnp.where(condition, 1.0, 0.0)


def fold_columns(spectrum):
    source = iota((EX, 128), 0)
    lane = iota((EX, 128), 1)
    folds = []
    for sign in (1.0, -1.0):
        for odd in (0, 1):
            kx = 2 * lane + odd
            fold = indicator(source == kx) + sign * indicator(source == EX - kx)
            if sign < 0 and not odd:
                fold = jnp.where(lane == 0, indicator(source == HALF_X), fold)
            folds.append(fold)
    fold = jnp.concatenate(folds, axis=1).astype(jnp.bfloat16)
    high, low = split(spectrum * (1.0 / (EY * EX)))
    return dot(high, fold) + dot(low, fold)


def fold_rows(folded, even_ref, cross_ref):
    high, low = split(folded)
    ky = iota((HALF_Y, EY), 0)
    row = iota((HALF_Y, EY), 1)
    straight = indicator(row == ky)
    mirrored = indicator(row == EY - ky)
    sums = (straight + mirrored).astype(jnp.bfloat16)
    gaps = jnp.where(ky == 0, 0.0, straight - mirrored).astype(jnp.bfloat16)
    even = dot(sums, high[:, :384]) + dot(sums, low[:, :384])
    cross = dot(gaps, high[:, 256:]) + dot(gaps, low[:, 256:])
    first_row = iota((HALF_Y, 128), 0) == 0
    first_lane = iota((HALF_Y, 128), 1) == 0
    middle = folded[HALF_Y : HALF_Y + 1]
    for slot, group in ((0, 0), (1, 0), (2, 1), (3, 1)):
        upper = even[:, 128 * group : 128 * group + 128]
        edge = jnp.broadcast_to(middle[:, 128 * group : 128 * group + 128], (HALF_Y, 128))
        if slot == 1:
            upper = jnp.where(first_lane, even[:, 256:384], upper)
            edge = jnp.where(first_lane, jnp.broadcast_to(middle[:, 256:384], (HALF_Y, 128)), edge)
        even_ref[0:HALF_Y, pl.ds(128 * slot, 128)] = upper
        even_ref[HALF_Y:EY, pl.ds(128 * slot, 128)] = jnp.where(first_row, edge, upper)
    cross_ref[:, 0:128] = jnp.where(first_lane, 0.0, cross[:, :128])
    cross_ref[:, 128:256] = cross[:, 128:]


def kernel(
    n_ty,
    n_tx,
    noise_ref,
    spectrum_ref,
    forward_ref,
    back_ref,
    columns_ref,
    turned_ref,
    out_ref,
    window,
    spectrum,
    forward,
    back,
    columns,
    turned,
    even,
    cross,
    staged,
    blended,
    side,
    from_remote,
    from_sibling,
    from_side,
    from_corner,
    local_sem,
    send_sem,
    recv_sem,
):
    me_y = lax.axis_index("ty")
    me_x = lax.axis_index("tx")
    core = lax.rem(me_y, 2)
    sibling_y = me_y + 1 - 2 * core
    remote_y = lax.rem(me_y + 2 * core - 1 + n_ty, n_ty)
    left_x = lax.rem(me_x + n_tx - 1, n_tx)
    right_x = lax.rem(me_x + 1, n_tx)

    sibling = (sibling_y, me_x)
    remote = (remote_y, me_x)
    left = (me_y, left_x)
    right = (me_y, right_x)
    corner_left = (remote_y, left_x)
    corner_right = (remote_y, right_x)
    partners = (remote, corner_left, corner_right, left, right, sibling)

    barrier = pltpu.get_barrier_semaphore()
    for partner in partners:
        pl.semaphore_signal(barrier, inc=1, device_id=partner, device_id_type=MESH)

    def local(source, target, index):
        copy = pltpu.make_async_copy(source, target, local_sem.at[index])
        copy.start()
        return copy

    own = window.at[1, :, pl.ds(MARGIN, BLOCK)]
    load_noise = local(noise_ref, own, 0)
    load_spectrum = local(spectrum_ref, spectrum, 1)
    slots = (2 * core, 1, 2 - 2 * core)
    load_tables = [local(forward_ref.at[slots[i]], forward.at[i], 2 + i) for i in range(3)]
    load_columns = local(columns_ref, columns, 5)
    load_turned = local(turned_ref, turned, 9)
    load_back = [local(back_ref.at[slots[i]], back.at[i], 6 + i) for i in range(3)]

    load_noise.wait()
    load_spectrum.wait()
    folded = fold_columns(spectrum[...])
    spectrum[...] = folded
    pl.semaphore_wait(barrier, len(partners))

    def send(source, target, index, device):
        copy = pltpu.make_async_remote_copy(
            src_ref=source,
            dst_ref=target,
            send_sem=send_sem.at[index],
            recv_sem=recv_sem.at[index],
            device_id=device,
            device_id_type=MESH,
        )
        copy.start()
        return copy

    left_strip = pl.ds(0, MARGIN)
    left_half = pl.ds(MARGIN, MARGIN)
    right_half = pl.ds(2 * MARGIN, MARGIN)
    right_strip = pl.ds(3 * MARGIN, MARGIN)
    centre = pl.ds(MARGIN, BLOCK)

    to_sibling = send(own, window.at[2, :, centre], 5, sibling)
    to_left = send(window.at[1, :, left_half], window.at[1, :, right_strip], 1, left)
    to_corner_left = send(window.at[1, :, left_half], window.at[0, :, right_strip], 4, corner_left)
    to_right = send(window.at[1, :, right_half], window.at[1, :, left_strip], 0, right)
    to_remote = send(own, window.at[0, :, centre], 2, remote)
    to_corner_right = send(window.at[1, :, right_half], window.at[0, :, left_strip], 3, corner_right)

    fold_rows(spectrum[...], even, cross)
    for load in load_tables:
        load.wait()
    load_columns.wait()

    def to_waves(rows):
        lower, upper = rows[:, :HALF_X], rows[:, HALF_X:]
        return jnp.concatenate(
            [
                three(split(lower + upper), (columns[0, 0], columns[1, 0])),
                three(split(lower - upper), (columns[0, 1], columns[1, 1])),
            ],
            axis=1,
        )

    position = iota((1, HALF_X), 1).astype(jnp.float32) + 0.5
    rising = position * (1.0 / HALF_X)
    falling = 1.0 - rising

    def from_waves(waves):
        straight = three(split(waves[:, :HALF_X]), (turned[0, 0], turned[1, 0]))
        crossed = three(split(waves[:, HALF_X:]), (turned[0, 1], turned[1, 1]))
        return (straight + crossed) * rising, (straight - crossed) * falling

    to_right.wait_recv()
    pass_left = send(window.at[1, :, left_strip], window.at[2, :, left_strip], 6, sibling)
    to_left.wait_recv()
    pass_right = send(window.at[1, :, right_strip], window.at[2, :, right_strip], 7, sibling)
    own_waves = split(to_waves(window[1]))
    staged[...] = three((forward[1, 0], forward[1, 1]), own_waves)
    to_sibling.wait_recv()
    pass_left.wait_recv()
    pass_right.wait_recv()
    sibling_waves = split(to_waves(window[2]))
    for load in (*load_back, load_turned):
        load.wait()
    to_remote.wait_recv()
    to_corner_right.wait_recv()
    to_corner_left.wait_recv()
    remote_waves = split(to_waves(window[0]))
    pairs = ((forward[2, 0], forward[2, 1], sibling_waves), (forward[0, 0], forward[0, 1], remote_waves))
    waves = staged[...] + dot(
        jnp.concatenate([t for high, low, _ in pairs for t in (high, high, low)], axis=1),
        jnp.concatenate([w for _, _, (high, low) in pairs for w in (high, low, high)], axis=0),
    )

    halves = []
    for parity in range(2):
        part = waves[:, 256 * parity : 256 * parity + 256]
        mixed = cross[:, pl.ds(128 * parity, 128)]
        real_c, real_s = part[:HALF_Y, :128], part[:HALF_Y, 128:]
        imag_c, imag_s = part[HALF_Y:, :128], part[HALF_Y:, 128:]
        shift = jnp.concatenate(
            [
                jnp.concatenate([mixed * imag_s, -(mixed * imag_c)], axis=1),
                jnp.concatenate([-(mixed * real_s), mixed * real_c], axis=1),
            ],
            axis=0,
        )
        halves.append(part * even[:, pl.ds(256 * parity, 256)] + shift)
    product = split(jnp.concatenate(halves, axis=1))

    def rows_of(slot):
        return three((back[slot, 0], back[slot, 1]), product)

    low_half, high_half = pl.ds(0, HALF_X), pl.ds(HALF_X, HALF_X)
    blended[0, :, low_half], blended[0, :, high_half] = from_waves(rows_of(0))
    add_remote = send(blended.at[0, :, centre], from_remote, 8, remote)
    blended[2] = rows_of(2)
    add_sibling = send(blended.at[2], from_sibling, 11, sibling)
    add_corner_left = send(blended.at[0, :, left_strip], from_corner.at[1], 9, corner_left)
    add_corner_right = send(blended.at[0, :, right_strip], from_corner.at[0], 10, corner_right)
    blended[1] = rows_of(1)
    add_sibling.wait_recv()
    low, high = from_waves(blended[1] + from_sibling[...])
    side[0] = low[:, :MARGIN]
    add_left = send(side.at[0], from_side.at[1], 12, left)
    side[1] = high[:, MARGIN:]
    add_right = send(side.at[1], from_side.at[0], 13, right)
    middle = jnp.concatenate([low[:, MARGIN:], high[:, :MARGIN]], axis=1)
    add_remote.wait_recv()
    middle = middle + from_remote[...]
    add_corner_left.wait_recv()
    add_corner_right.wait_recv()
    middle = middle + jnp.concatenate([from_corner[0], from_corner[1]], axis=1)
    add_left.wait_recv()
    add_right.wait_recv()
    out_ref[...] = middle + jnp.concatenate([from_side[0], from_side[1]], axis=1)
    for copy in (
        to_right,
        to_left,
        to_remote,
        to_corner_right,
        to_corner_left,
        to_sibling,
        pass_left,
        pass_right,
        add_remote,
        add_corner_left,
        add_corner_right,
        add_sibling,
        add_left,
        add_right,
    ):
        copy.wait_send()


def per_device(n_ty, n_tx, noise, root_spectrum):
    constants = [jnp.asarray(table) for table in tables()]
    anywhere = pl.BlockSpec(memory_space=pl.ANY)
    f32 = jnp.float32
    bf16 = jnp.bfloat16
    return pl.pallas_call(
        functools.partial(kernel, n_ty, n_tx),
        out_shape=pltpu.VMEM(noise.shape, f32),
        in_specs=[anywhere] * 6,
        out_specs=pl.BlockSpec(memory_space=pltpu.VMEM),
        scratch_shapes=[
            pltpu.VMEM((3, MARGIN, EX), f32),
            pltpu.VMEM((EY, EX), f32),
            pltpu.VMEM((3, 2, EY, MARGIN), bf16),
            pltpu.VMEM((3, 2, MARGIN, EY), bf16),
            pltpu.VMEM((2, 2, HALF_X, HALF_X), bf16),
            pltpu.VMEM((2, 2, HALF_X, HALF_X), bf16),
            pltpu.VMEM((EY, EX), f32),
            pltpu.VMEM((HALF_Y, HALF_X), f32),
            pltpu.VMEM((EY, EX), f32),
            pltpu.VMEM((3, MARGIN, EX), f32),
            pltpu.VMEM((2, MARGIN, MARGIN), f32),
            pltpu.VMEM((MARGIN, BLOCK), f32),
            pltpu.VMEM((MARGIN, EX), f32),
            pltpu.VMEM((2, MARGIN, MARGIN), f32),
            pltpu.VMEM((2, MARGIN, MARGIN), f32),
            pltpu.SemaphoreType.DMA((10,)),
            pltpu.SemaphoreType.DMA((14,)),
            pltpu.SemaphoreType.DMA((14,)),
        ],
        compiler_params=pltpu.CompilerParams(collective_id=0, has_side_effects=True),
        name="field_tile",
    )(noise, root_spectrum, *constants)


def solution(mesh):
    placed = (P("ty", "tx"), P())
    body = functools.partial(per_device, mesh.shape["ty"], mesh.shape["tx"])
    return jax.shard_map(
        body, mesh=mesh, in_specs=placed, out_specs=P("ty", "tx"), check_vma=False
    )
```

```python
import functools
import math

import jax
import jax.numpy as jnp
import numpy as np
from jax import lax
from jax.experimental import pallas as pl
from jax.experimental.pallas import tpu as pltpu
from jax.sharding import PartitionSpec as P

MARGIN = 128
EY = 384
EX = 512
BLOCK = 256
HALF_Y = EY // 2
HALF_X = EX // 2
MESH = pl.DeviceIdType.MESH


def split_table(table):
    high = table.astype(jnp.bfloat16)
    low = (table - high.astype(np.float64)).astype(jnp.bfloat16)
    return np.stack([high, low])


def row_basis():
    ky = np.arange(HALF_Y)[:, None]
    y = np.arange(EY)[None, :]
    angle = 2.0 * math.pi * (ky * y % EY) / EY
    lower = -np.sin(angle)
    lower[0] = np.cos(math.pi * np.arange(EY))
    return np.concatenate([np.cos(angle), lower])


def column_basis():
    x = np.arange(HALF_X)[:, None]
    bases = []
    for odd in (0, 1):
        kx = 2 * np.arange(HALF_X // 2)[None, :] + odd
        angle = 2.0 * math.pi * (kx * x % EX) / EX
        sine = np.sin(angle)
        if not odd:
            sine[:, 0] = np.cos(math.pi * np.arange(HALF_X))
        bases.append(np.concatenate([np.cos(angle), sine], axis=1))
    return np.stack(bases)


def row_weights():
    knots = (np.arange(EY) + 0.5) / MARGIN
    return np.where(
        knots < 1.0,
        0.5 * knots * knots,
        np.where(
            knots < 2.0,
            0.5 * (-2.0 * knots * knots + 6.0 * knots - 3.0),
            0.5 * (3.0 - knots) * (3.0 - knots),
        ),
    )


def tables():
    rows = row_basis()
    forward = split_table(rows)
    forward = forward.reshape(2, EY, 3, MARGIN).transpose(2, 0, 1, 3)
    back = split_table((rows * row_weights()[None, :]).T)
    back = back.reshape(2, 3, MARGIN, EY).transpose(1, 0, 2, 3)
    columns = split_table(column_basis())
    turned = columns.transpose(0, 1, 3, 2)
    return [np.ascontiguousarray(table) for table in (forward, back, columns, turned)]


def split(value):
    high = value.astype(jnp.bfloat16)
    return high, (value - high.astype(jnp.float32)).astype(jnp.bfloat16)


def dot(left, right):
    return jnp.dot(left, right, preferred_element_type=jnp.float32)


def three(left, right):
    return dot(
        jnp.concatenate([left[0], left[0], left[1]], axis=1),
        jnp.concatenate([right[0], right[1], right[0]], axis=0),
    )


def iota(shape, dim):
    return lax.broadcasted_iota(jnp.int32, shape, dim)


def indicator(condition):
    return jnp.where(condition, 1.0, 0.0)


def fold_columns(spectrum):
    source = iota((EX, 128), 0)
    lane = iota((EX, 128), 1)
    folds = []
    for sign in (1.0, -1.0):
        for odd in (0, 1):
            kx = 2 * lane + odd
            fold = indicator(source == kx) + sign * indicator(source == EX - kx)
            if sign < 0 and not odd:
                fold = jnp.where(lane == 0, indicator(source == HALF_X), fold)
            folds.append(fold)
    fold = jnp.concatenate(folds, axis=1).astype(jnp.bfloat16)
    high, low = split(spectrum * (1.0 / (EY * EX)))
    return dot(high, fold) + dot(low, fold)


def fold_rows(folded, even_ref, cross_ref):
    high, low = split(folded)
    ky = iota((HALF_Y, EY), 0)
    row = iota((HALF_Y, EY), 1)
    straight = indicator(row == ky)
    mirrored = indicator(row == EY - ky)
    sums = (straight + mirrored).astype(jnp.bfloat16)
    gaps = jnp.where(ky == 0, 0.0, straight - mirrored).astype(jnp.bfloat16)
    even = dot(sums, high[:, :384]) + dot(sums, low[:, :384])
    cross = dot(gaps, high[:, 256:]) + dot(gaps, low[:, 256:])
    first_row = iota((HALF_Y, 128), 0) == 0
    first_lane = iota((HALF_Y, 128), 1) == 0
    middle = folded[HALF_Y : HALF_Y + 1]
    for slot, group in ((0, 0), (1, 0), (2, 1), (3, 1)):
        upper = even[:, 128 * group : 128 * group + 128]
        edge = jnp.broadcast_to(middle[:, 128 * group : 128 * group + 128], (HALF_Y, 128))
        if slot == 1:
            upper = jnp.where(first_lane, even[:, 256:384], upper)
            edge = jnp.where(first_lane, jnp.broadcast_to(middle[:, 256:384], (HALF_Y, 128)), edge)
        even_ref[0:HALF_Y, pl.ds(128 * slot, 128)] = upper
        even_ref[HALF_Y:EY, pl.ds(128 * slot, 128)] = jnp.where(first_row, edge, upper)
    cross_ref[:, 0:128] = jnp.where(first_lane, 0.0, cross[:, :128])
    cross_ref[:, 128:256] = cross[:, 128:]


def kernel(
    n_ty,
    n_tx,
    noise_ref,
    spectrum_ref,
    forward_ref,
    back_ref,
    columns_ref,
    turned_ref,
    out_ref,
    window,
    spectrum,
    forward,
    back,
    columns,
    turned,
    even,
    cross,
    staged,
    blended,
    side,
    from_remote,
    from_sibling,
    from_side,
    from_corner,
    local_sem,
    send_sem,
    recv_sem,
):
    me_y = lax.axis_index("ty")
    me_x = lax.axis_index("tx")
    core = lax.rem(me_y, 2)
    sibling_y = me_y + 1 - 2 * core
    remote_y = lax.rem(me_y + 2 * core - 1 + n_ty, n_ty)
    left_x = lax.rem(me_x + n_tx - 1, n_tx)
    right_x = lax.rem(me_x + 1, n_tx)

    sibling = (sibling_y, me_x)
    remote = (remote_y, me_x)
    left = (me_y, left_x)
    right = (me_y, right_x)
    corner_left = (remote_y, left_x)
    corner_right = (remote_y, right_x)
    partners = (remote, corner_left, corner_right, left, right, sibling)

    barrier = pltpu.get_barrier_semaphore()
    for partner in partners:
        pl.semaphore_signal(barrier, inc=1, device_id=partner, device_id_type=MESH)

    def local(source, target, index):
        copy = pltpu.make_async_copy(source, target, local_sem.at[index])
        copy.start()
        return copy

    own = window.at[1, :, pl.ds(MARGIN, BLOCK)]
    load_noise = local(noise_ref, own, 0)
    load_spectrum = local(spectrum_ref, spectrum, 1)
    slots = (2 * core, 1, 2 - 2 * core)
    load_tables = [local(forward_ref.at[slots[i]], forward.at[i], 2 + i) for i in range(3)]
    load_columns = local(columns_ref, columns, 5)
    load_turned = local(turned_ref, turned, 9)
    load_back = [local(back_ref.at[slots[i]], back.at[i], 6 + i) for i in range(3)]

    load_noise.wait()
    load_spectrum.wait()
    folded = fold_columns(spectrum[...])
    spectrum[...] = folded
    pl.semaphore_wait(barrier, len(partners))

    def send(source, target, index, device):
        copy = pltpu.make_async_remote_copy(
            src_ref=source,
            dst_ref=target,
            send_sem=send_sem.at[index],
            recv_sem=recv_sem.at[index],
            device_id=device,
            device_id_type=MESH,
        )
        copy.start()
        return copy

    left_strip = pl.ds(0, MARGIN)
    left_half = pl.ds(MARGIN, MARGIN)
    right_half = pl.ds(2 * MARGIN, MARGIN)
    right_strip = pl.ds(3 * MARGIN, MARGIN)
    centre = pl.ds(MARGIN, BLOCK)

    to_sibling = send(own, window.at[2, :, centre], 5, sibling)
    to_left = send(window.at[1, :, left_half], window.at[1, :, right_strip], 1, left)
    to_corner_left = send(window.at[1, :, left_half], window.at[0, :, right_strip], 4, corner_left)
    to_right = send(window.at[1, :, right_half], window.at[1, :, left_strip], 0, right)
    to_remote = send(own, window.at[0, :, centre], 2, remote)
    to_corner_right = send(window.at[1, :, right_half], window.at[0, :, left_strip], 3, corner_right)

    fold_rows(spectrum[...], even, cross)
    for load in load_tables:
        load.wait()
    load_columns.wait()

    def to_waves(rows):
        lower, upper = rows[:, :HALF_X], rows[:, HALF_X:]
        return jnp.concatenate(
            [
                three(split(lower + upper), (columns[0, 0], columns[1, 0])),
                three(split(lower - upper), (columns[0, 1], columns[1, 1])),
            ],
            axis=1,
        )

    position = iota((1, HALF_X), 1).astype(jnp.float32) + 0.5
    rising = position * (1.0 / HALF_X)
    falling = 1.0 - rising

    def from_waves(waves):
        straight = three(split(waves[:, :HALF_X]), (turned[0, 0], turned[1, 0]))
        crossed = three(split(waves[:, HALF_X:]), (turned[0, 1], turned[1, 1]))
        return (straight + crossed) * rising, (straight - crossed) * falling

    to_left.wait_recv()
    pass_right = send(window.at[1, :, right_strip], window.at[2, :, right_strip], 7, sibling)
    to_right.wait_recv()
    pass_left = send(window.at[1, :, left_strip], window.at[2, :, left_strip], 6, sibling)
    own_waves = split(to_waves(window[1]))
    staged[...] = three((forward[1, 0], forward[1, 1]), own_waves)
    to_sibling.wait_recv()
    pass_left.wait_recv()
    pass_right.wait_recv()
    sibling_waves = split(to_waves(window[2]))
    for load in (*load_back, load_turned):
        load.wait()
    to_remote.wait_recv()
    to_corner_right.wait_recv()
    to_corner_left.wait_recv()
    remote_waves = split(to_waves(window[0]))
    pairs = ((forward[2, 0], forward[2, 1], sibling_waves), (forward[0, 0], forward[0, 1], remote_waves))
    waves = staged[...] + dot(
        jnp.concatenate([t for high, low, _ in pairs for t in (high, high, low)], axis=1),
        jnp.concatenate([w for _, _, (high, low) in pairs for w in (high, low, high)], axis=0),
    )

    halves = []
    for parity in range(2):
        part = waves[:, 256 * parity : 256 * parity + 256]
        mixed = cross[:, pl.ds(128 * parity, 128)]
        real_c, real_s = part[:HALF_Y, :128], part[:HALF_Y, 128:]
        imag_c, imag_s = part[HALF_Y:, :128], part[HALF_Y:, 128:]
        shift = jnp.concatenate(
            [
                jnp.concatenate([mixed * imag_s, -(mixed * imag_c)], axis=1),
                jnp.concatenate([-(mixed * real_s), mixed * real_c], axis=1),
            ],
            axis=0,
        )
        halves.append(part * even[:, pl.ds(256 * parity, 256)] + shift)
    product = split(jnp.concatenate(halves, axis=1))

    def rows_of(slot):
        return three((back[slot, 0], back[slot, 1]), product)

    low_half, high_half = pl.ds(0, HALF_X), pl.ds(HALF_X, HALF_X)
    blended[0, :, low_half], blended[0, :, high_half] = from_waves(rows_of(0))
    add_remote = send(blended.at[0, :, centre], from_remote, 8, remote)
    blended[2] = rows_of(2)
    add_sibling = send(blended.at[2], from_sibling, 11, sibling)
    add_corner_left = send(blended.at[0, :, left_strip], from_corner.at[1], 9, corner_left)
    add_corner_right = send(blended.at[0, :, right_strip], from_corner.at[0], 10, corner_right)
    blended[1] = rows_of(1)
    add_sibling.wait_recv()
    low, high = from_waves(blended[1] + from_sibling[...])
    side[0] = low[:, :MARGIN]
    add_left = send(side.at[0], from_side.at[1], 12, left)
    side[1] = high[:, MARGIN:]
    add_right = send(side.at[1], from_side.at[0], 13, right)
    middle = jnp.concatenate([low[:, MARGIN:], high[:, :MARGIN]], axis=1)
    add_remote.wait_recv()
    middle = middle + from_remote[...]
    add_corner_left.wait_recv()
    add_corner_right.wait_recv()
    middle = middle + jnp.concatenate([from_corner[0], from_corner[1]], axis=1)
    add_left.wait_recv()
    add_right.wait_recv()
    out_ref[...] = middle + jnp.concatenate([from_side[0], from_side[1]], axis=1)
    for copy in (
        to_right,
        to_left,
        to_remote,
        to_corner_right,
        to_corner_left,
        to_sibling,
        pass_left,
        pass_right,
        add_remote,
        add_corner_left,
        add_corner_right,
        add_sibling,
        add_left,
        add_right,
    ):
        copy.wait_send()


def per_device(n_ty, n_tx, noise, root_spectrum):
    constants = [jnp.asarray(table) for table in tables()]
    anywhere = pl.BlockSpec(memory_space=pl.ANY)
    f32 = jnp.float32
    bf16 = jnp.bfloat16
    return pl.pallas_call(
        functools.partial(kernel, n_ty, n_tx),
        out_shape=pltpu.VMEM(noise.shape, f32),
        in_specs=[anywhere] * 6,
        out_specs=pl.BlockSpec(memory_space=pltpu.VMEM),
        scratch_shapes=[
            pltpu.VMEM((3, MARGIN, EX), f32),
            pltpu.VMEM((EY, EX), f32),
            pltpu.VMEM((3, 2, EY, MARGIN), bf16),
            pltpu.VMEM((3, 2, MARGIN, EY), bf16),
            pltpu.VMEM((2, 2, HALF_X, HALF_X), bf16),
            pltpu.VMEM((2, 2, HALF_X, HALF_X), bf16),
            pltpu.VMEM((EY, EX), f32),
            pltpu.VMEM((HALF_Y, HALF_X), f32),
            pltpu.VMEM((EY, EX), f32),
            pltpu.VMEM((3, MARGIN, EX), f32),
            pltpu.VMEM((2, MARGIN, MARGIN), f32),
            pltpu.VMEM((MARGIN, BLOCK), f32),
            pltpu.VMEM((MARGIN, EX), f32),
            pltpu.VMEM((2, MARGIN, MARGIN), f32),
            pltpu.VMEM((2, MARGIN, MARGIN), f32),
            pltpu.SemaphoreType.DMA((10,)),
            pltpu.SemaphoreType.DMA((14,)),
            pltpu.SemaphoreType.DMA((14,)),
        ],
        compiler_params=pltpu.CompilerParams(collective_id=0, has_side_effects=True),
        name="field_tile",
    )(noise, root_spectrum, *constants)


def solution(mesh):
    placed = (P("ty", "tx"), P())
    body = functools.partial(per_device, mesh.shape["ty"], mesh.shape["tx"])
    return jax.shard_map(
        body, mesh=mesh, in_specs=placed, out_specs=P("ty", "tx"), check_vma=False
    )
```
